512 devices in a mesh: rep: 2 (over y), seq: 16 (over z), head: 8 (over x), sub: 2 (over core).
Axes of the slice: x: 8, y: 2, z: 16, core: 2. Of those that a mesh axis runs over, the one named last changes fastest.
The devices are a block of a 8x8x16 slice.
Arguments:
- queries: bfloat16 [32, 8192], P('rep', 'head'), parts along dimension 0, may hold values from -4.5 to 4.5
- key_cache: bfloat16 [4096, 128, 1024], P(('rep', 'seq', 'sub'), None, 'head'), parts along dimension 0, may hold values from -4.5 to 4.5
- value_cache: bfloat16 [4096, 128, 1024], P(('rep', 'seq', 'sub'), None, 'head'), parts along dimension 0, may hold values from -6 to 6
- seq_lengths: int32 [32], P('rep'), parts along dimension 0, may hold values from 513 to 32768, as said below
- slot_owner: int32 [4096], P(('rep', 'seq', 'sub')), parts along dimension 0, may hold values from 0 to 15, as said below
- slot_page: int32 [4096], P(('rep', 'seq', 'sub')), parts along dimension 0, may hold values from 0 to 255, as said below
- out_weight: bfloat16 [8192, 8192], P('head', ('seq', 'sub')), may hold values from -0.0625 to 0.0625
Outputs:
- projected: bfloat16 [32, 8192], P('rep', ('seq', 'sub')), parts along dimension 0
The draws below stay inside these ranges and needn't reach their ends.
There are 2 independent parts, one for each index of `rep`. The reference program is written for one: setup_inputs(seed, part) draws one part's arguments, and reference() takes and returns one part's arrays. A program takes and returns all parts, laid end to end along the dimension named above; an argument that names none is the same for every part. Nothing has to cross between parts.
Inputs may be any that keep to these rules, and one draw needn't show every extreme that they name: `slot_owner`: every sequence holds 5 to 256 pages, and some sequence exactly 256; its pages are numbered 0 upward and each stands in exactly one cache page; every cache page is used; a sequence's pages occupy consecutive cache pages. slot_page[s] < ceil(seq_lengths[slot_owner[s]] / 128), and every page below that count is present. seq_lengths[b] lies in the last of its sequence's pages.
All inputs are finite; a program needn't handle non-finite values.
Results may differ from the reference program's by a relative error of at most 0.0055.
Values may be sent and summed in bfloat16 or wider, within the bound.
A program may use at most 64 MiB of HBM per device.

```python
import jax
import jax.numpy as jnp
from jax import lax

D = 8192
HQ = 64
KVH = 8
DH = 128
PAGE = 128
PAGE_DEV = 64
SLOTS = 2048
BATCH = 16
MAX_PAGES = 256


min_pages = 5


def page_layout(key):
    longest = jax.random.randint(jax.random.fold_in(key, 13), (), 0, BATCH).astype(jnp.int32)
    indices = jnp.arange(BATCH, dtype=jnp.int32)
    others = (indices != longest).astype(jnp.int32)
    roots = jax.random.randint(jax.random.fold_in(key, 11), (BATCH,), 1, 8).astype(jnp.int32)
    weights = roots * roots * roots * others
    spare = SLOTS - MAX_PAGES - (BATCH - 1) * min_pages
    room_cap = MAX_PAGES - min_pages
    extra = spare * weights // jnp.sum(weights)
    extra = jnp.minimum(extra, room_cap) * others
    leftover = spare - jnp.sum(extra)
    room = (room_cap - extra) * others
    before = jnp.cumsum(room) - room
    extra = extra + jnp.clip(leftover - before, 0, room)
    pages = jnp.where(others == 1, min_pages + extra, MAX_PAGES).astype(jnp.int32)
    ends = jnp.cumsum(pages).astype(jnp.int32)
    starts = ends - pages
    slot_index = jnp.arange(SLOTS, dtype=jnp.int32)
    owners = jnp.sum((slot_index[:, None] >= ends[None, :]).astype(jnp.int32), axis=1).astype(jnp.int32)
    page_number = (slot_index - starts[owners]).astype(jnp.int32)
    tails = jax.random.randint(jax.random.fold_in(key, 12), (BATCH,), 1, PAGE + 1).astype(jnp.int32)
    tails = jnp.where(others == 1, tails, PAGE)
    lengths = ((pages - 1) * PAGE + tails).astype(jnp.int32)
    return (lengths, owners, page_number)


def draw_seq_lengths(key, part):
    return page_layout(key)[0]


def draw_slot_owner(key, part):
    return page_layout(key)[1]


def draw_slot_page(key, part):
    return page_layout(key)[2]


def draw_queries(key, part):
    values = jnp.clip(jax.random.normal(jax.random.fold_in(key, 41), (BATCH, HQ * DH), jnp.float32), -4.5, 4.5)
    return values.astype(jnp.bfloat16)


def draw_key_cache(key, part):
    values = jnp.clip(jax.random.normal(jax.random.fold_in(key, 51), (SLOTS, PAGE, KVH * DH), jnp.float32), -4.5, 4.5)
    return values.astype(jnp.bfloat16)


def block_levels(key, dims, split, least, high):
    factor_of = 1.0
    for position, parts in split:
        heights = jax.random.uniform(jax.random.fold_in(jax.random.fold_in(key, 6), position), (parts,), jnp.float32, least / len(split), high / len(split))
        factor_of = factor_of * jnp.repeat(jnp.exp(heights), dims[position] // parts).reshape((-1,) + (1,) * (len(dims) - 1 - position))
    return factor_of


def gaussian(own_key, extent, width, bound, shards=(), kind=jnp.bfloat16):
    result = width * jax.random.normal(own_key, extent, jnp.float32)
    if shards:
        result = result * block_levels(own_key, extent, shards, -0.22, 0.18)
    return jnp.clip(result, -bound, bound).astype(kind)


def setup_inputs(seed: int = 0, part: int = 0) -> dict:
    key_of = jax.random.split(jax.random.key(seed), 8)
    part_splits = jax.random.split(jax.random.fold_in(key_of[7], part), 8)
    return {
        "queries": draw_queries(jax.random.fold_in(jax.random.fold_in(key_of[7], part), 71), part),
        "key_cache": draw_key_cache(jax.random.fold_in(jax.random.fold_in(key_of[7], part), 71), part),
        "value_cache": gaussian(part_splits[2], (SLOTS, PAGE, KVH * DH), 1.0, 6.0, ((0, 32), (2, 8))),
        "seq_lengths": draw_seq_lengths(jax.random.fold_in(jax.random.fold_in(key_of[7], part), 71), part),
        "slot_owner": draw_slot_owner(jax.random.fold_in(jax.random.fold_in(key_of[7], part), 71), part),
        "slot_page": draw_slot_page(jax.random.fold_in(jax.random.fold_in(key_of[7], part), 71), part),
        "out_weight": gaussian(key_of[6], (HQ * DH, D), (HQ * DH) ** -0.5, 0.0625, ((0, 8), (1, 32))),
    }


neg_fill = -1e+30

def reference(queries, key_cache, value_cache, seq_lengths, slot_owner, slot_page, out_weight):
    per_group = HQ // KVH
    blocks = SLOTS // PAGE_DEV
    query_heads = queries.astype(jnp.float32).reshape(BATCH, KVH, per_group, DH)
    valid = jnp.clip(seq_lengths[slot_owner] - slot_page * PAGE, 0, PAGE).astype(jnp.int32)
    positions = jnp.arange(PAGE, dtype=jnp.int32)

    def one_block(block):
        key_tiles, value_tiles, owners, counts = block
        picked = query_heads[owners]
        key_float = key_tiles.astype(jnp.float32).reshape(PAGE_DEV, PAGE, KVH, DH)
        value_float = value_tiles.astype(jnp.float32).reshape(PAGE_DEV, PAGE, KVH, DH)
        scores = jnp.einsum('sgjd,stgd->sgjt', picked, key_float, precision=lax.Precision.HIGHEST)
        scores = scores * (1.0 / jnp.sqrt(jnp.float32(DH)))
        live = (positions[None, :] < counts[:, None])[:, None, None, :]
        scores = jnp.where(live, scores, neg_fill)
        page_peak = lax.optimization_barrier(jnp.max(scores, axis=-1))
        probs = jnp.exp(scores - page_peak[..., None]).astype(jnp.bfloat16)
        prob_float = probs.astype(jnp.float32)
        page_mass = lax.optimization_barrier(jnp.sum(prob_float, axis=-1))
        page_out = jnp.einsum('sgjt,stgd->sgjd', prob_float, value_float, precision=lax.Precision.HIGHEST)
        return (page_peak, page_mass, page_out)
    page_peak, page_mass, page_out = lax.map(one_block, (key_cache.reshape(blocks, PAGE_DEV, PAGE, KVH * DH), value_cache.reshape(blocks, PAGE_DEV, PAGE, KVH * DH), slot_owner.reshape(blocks, PAGE_DEV), valid.reshape(blocks, PAGE_DEV)))
    page_peak = page_peak.reshape(SLOTS, KVH, per_group)
    page_mass = page_mass.reshape(SLOTS, KVH, per_group)
    page_out = page_out.reshape(SLOTS, KVH, per_group, DH)
    owner_hits = slot_owner[None, :] == jnp.arange(BATCH, dtype=jnp.int32)[:, None]
    seq_peak = lax.optimization_barrier(jnp.max(jnp.where(owner_hits[:, :, None, None], page_peak[None], neg_fill), axis=1))
    factor = jnp.exp(page_peak - seq_peak[slot_owner])
    seq_mass = jax.ops.segment_sum(page_mass * factor, slot_owner, num_segments=BATCH)
    seq_out = jax.ops.segment_sum(page_out * factor[..., None], slot_owner, num_segments=BATCH)
    attention = (seq_out / seq_mass[..., None]).reshape(BATCH, HQ * DH).astype(jnp.bfloat16)
    return jnp.dot(attention, out_weight, preferred_element_type=jnp.float32).astype(jnp.bfloat16)
```

```python
import functools

import jax
import jax.numpy as jnp
from jax import lax
from jax.experimental import pallas as pl
from jax.experimental.pallas import tpu as pltpu
from jax.sharding import PartitionSpec as P

DH = 128
PAGE = 128
NEG = -1e30
CHUNKS = 4
F32 = jnp.float32
BF16 = jnp.bfloat16
MESH = pl.DeviceIdType.MESH


def kernel(
    sizes,
    lengths,
    owners,
    numbers,
    owner_row,
    q_ref,
    k_hbm,
    v_hbm,
    w_hbm,
    out_ref,
    k_ref,
    v_ref,
    w_ref,
    q_rows,
    q_seq,
    peaks,
    masses,
    scaled,
    hits,
    seq_lse,
    lse_diag,
    part_out,
    part_lse,
    got_out,
    got_lse,
    half_out,
    half_lse,
    all_out,
    all_lse,
    att_rows,
    proj_mine,
    proj_all,
    k_sem,
    v_sem,
    w_sem,
    a_send,
    a_recv,
    b_send,
    b_recv,
    c_send,
    c_recv,
    far_sem,
):
    n_z, n_x, n_c = sizes
    batch, heads, slots = lengths.shape[0], q_ref.shape[1] // DH, owners.shape[0]
    half = n_z // 2
    near = half // 2
    z, x, c = lax.axis_index("seq"), lax.axis_index("head"), lax.axis_index("sub")
    rows = batch * heads
    per_chunk = slots // CHUNKS

    def ring(offset):
        return lax.rem(z + offset + n_z, n_z)

    def core(j):
        return lax.rem(c + j, n_c)

    loads = []
    for hbm, ref, sem in ((k_hbm, k_ref, k_sem), (v_hbm, v_ref, v_sem)):
        copies = []
        for i in range(CHUNKS):
            span = pl.ds(i * per_chunk, per_chunk)
            copies.append(pltpu.make_async_copy(hbm.at[span], ref.at[span], sem.at[i]))
        loads.append(copies)
    w_load = pltpu.make_async_copy(w_hbm, w_ref, w_sem)
    for copies in loads:
        for copy in copies:
            copy.start()
    w_load.start()

    barrier = pltpu.get_barrier_semaphore()
    greeted = 0
    for dz in range(-near, near + 1):
        for j in range(n_c):
            if dz or j:
                greeted += 1
                pl.semaphore_signal(
                    barrier, inc=1, device_id={"seq": ring(dz), "sub": core(j)}, device_id_type=MESH
                )
    for dx in range(1, n_x):
        greeted += 1
        pl.semaphore_signal(
            barrier, inc=1, device_id={"head": lax.rem(x + dx, n_x)}, device_id_type=MESH
        )

    lane = lax.broadcasted_iota(jnp.int32, (heads, rows), 1)
    sub = lax.broadcasted_iota(jnp.int32, (heads, rows), 0)
    diag = lane - sub

    for h in range(heads):
        q_rows[pl.ds(h, batch, stride=heads), :] = q_ref[:, h * DH : (h + 1) * DH].astype(F32)
    q_seq[...] = q_rows[...].reshape(batch, heads, DH)

    hit = (lax.broadcasted_iota(jnp.int32, (batch, slots), 0) == owner_row[...]).astype(BF16)
    spread_rows = lax.broadcasted_iota(jnp.int32, (slots, slots * heads), 0)
    spread_cols = lax.broadcasted_iota(jnp.int32, (slots, slots * heads), 1)
    spread = (spread_cols // heads == spread_rows).astype(BF16)
    wide = jnp.dot(hit, spread, preferred_element_type=F32)
    wide = jnp.broadcast_to(wide[:, None, :], (batch, heads, slots * heads))
    w_sub = lax.broadcasted_iota(jnp.int32, (batch, heads, slots * heads), 1)
    w_lane = lax.broadcasted_iota(jnp.int32, (batch, heads, slots * heads), 2)
    hits[...] = jnp.where(w_lane % heads == w_sub, wide, 0.0).reshape(rows, slots * heads).astype(BF16)

    scale = 1.0 / (float(DH) ** 0.5)
    pair_sub = lax.broadcasted_iota(jnp.int32, (2 * heads, PAGE), 0)
    pair_lane = lax.broadcasted_iota(jnp.int32, (2 * heads, PAGE), 1)
    first = pair_sub < heads

    probs = []
    top = jnp.full((heads, rows), NEG, F32)
    for i in range(CHUNKS):
        loads[0][i].wait()
        for pair in range(i * per_chunk // 2, (i + 1) * per_chunk // 2):
            a, b = 2 * pair, 2 * pair + 1
            own_a, own_b = owners[a], owners[b]
            q_pair = jnp.concatenate(
                [
                    q_seq[own_a],
                    q_seq[own_b],
                ],
                axis=0,
            ).astype(BF16)
            keys = k_ref[a : b + 1].reshape(2 * PAGE, DH)
            both = lax.dot_general(
                q_pair, keys, (((1,), (1,)), ((), ())), preferred_element_type=F32
            )
            scores = jnp.concatenate([both[:heads, :PAGE], both[heads:, PAGE:]], axis=0) * scale
            live_a = jnp.clip(lengths[own_a] - numbers[a] * PAGE, 0, PAGE)
            live_b = jnp.clip(lengths[own_b] - numbers[b] * PAGE, 0, PAGE)
            scores = jnp.where(pair_lane < jnp.where(first, live_a, live_b), scores, NEG)
            peak = jnp.max(scores, axis=1, keepdims=True)
            prob = jnp.exp(scores - peak).astype(BF16)
            mass = jnp.sum(prob.astype(F32), axis=1, keepdims=True)
            peak = jnp.broadcast_to(peak, (2 * heads, PAGE))
            mass = jnp.broadcast_to(mass, (2 * heads, PAGE))
            peaks[pl.ds(a * heads, 2 * heads), :] = peak
            masses[pl.ds(a * heads, 2 * heads), :] = mass
            probs.append(prob)
            top = jnp.maximum(top, jnp.where(diag == own_a * heads, peak[:heads], NEG))
            top = jnp.maximum(top, jnp.where(diag == own_b * heads, peak[heads:], NEG))

    def by_sequence(row_values):
        for b in range(batch):
            mine = jnp.max(
                jnp.where(lane // heads == b, row_values, 2 * NEG), axis=1, keepdims=True
            )
            seq_lse[b] = jnp.broadcast_to(mine, (heads, rows))

    by_sequence(top)
    total = jnp.zeros((heads, rows), F32)
    for s in range(slots):
        span = pl.ds(s * heads, heads)
        factor = jnp.exp(peaks[span, :] - seq_lse[owners[s]])
        total = total + jnp.where(diag == owners[s] * heads, factor * masses[span, :], 0.0)
    lse = jnp.where(total > 0.0, top + jnp.log(jnp.where(total > 0.0, total, 1.0)), NEG)
    by_sequence(lse)

    for b in range(batch):
        lse_diag[pl.ds(b * heads, heads), :] = jnp.where(lane % heads == sub, seq_lse[b], 0.0)
    tiled = lse_diag[pl.ds(0, batch, stride=heads), :]
    for h in range(1, heads):
        tiled = tiled + lse_diag[pl.ds(h, batch, stride=heads), :]
    part_lse[...] = tiled.reshape(batch, 1, rows)

    for i in range(CHUNKS):
        loads[1][i].wait()
        for pair in range(i * per_chunk // 2, (i + 1) * per_chunk // 2):
            a, b = 2 * pair, 2 * pair + 1
            prob = probs[pair]
            block = jnp.concatenate(
                [
                    jnp.where(first, prob, jnp.zeros_like(prob)),
                    jnp.where(first, jnp.zeros_like(prob), prob),
                ],
                axis=1,
            )
            values = v_ref[a : b + 1].reshape(2 * PAGE, DH)
            page_out = jnp.dot(block, values, preferred_element_type=F32)
            span = pl.ds(a * heads, 2 * heads)
            level = jnp.concatenate([seq_lse[owners[a]], seq_lse[owners[b]]], axis=0)
            factor = jnp.exp(peaks[span, :] - level)
            scaled[span, :] = (page_out * factor).astype(BF16)
    mine = jnp.dot(hits[...], scaled[...], preferred_element_type=F32)
    part_out[...] = mine.astype(BF16).reshape(batch, heads, DH)

    pl.semaphore_wait(barrier, greeted)
    for dz in (-near, near):
        pl.semaphore_signal(far_sem, inc=1, device_id={"seq": ring(dz)}, device_id_type=MESH)

    a_copies = []
    order = sorted(range(-near, near), key=lambda d: -abs(d))
    for dz in order:
        for j in range(n_c):
            target = lax.rem(ring(dz), half) * n_c + core(j)
            slot = (near - 1 - dz) * n_c + j
            if dz == 0 and j == 0:
                got_out[slot] = part_out[target]
                got_lse[pl.ds(slot, 1), :] = part_lse[target]
                continue
            for k, (src, dst) in enumerate(
                ((part_out.at[target], got_out.at[slot]), (part_lse.at[target], got_lse.at[pl.ds(slot, 1), :]))
            ):
                copy = pltpu.make_async_remote_copy(
                    src_ref=src,
                    dst_ref=dst,
                    send_sem=a_send.at[slot, k],
                    recv_sem=a_recv.at[slot, k],
                    device_id={"seq": ring(dz), "sub": core(j)},
                    device_id_type=MESH,
                )
                copy.start()
                a_copies.append(copy)
    for copy in a_copies:
        copy.wait_recv()

    sources = half * n_c
    levels = got_lse[...]
    peak = jnp.max(levels, axis=0, keepdims=True)
    weight = jnp.exp(levels - peak)
    norm = jnp.sum(weight, axis=0, keepdims=True)
    weight = weight / norm
    s_sub = lax.broadcasted_iota(jnp.int32, (sources, sources * heads), 0)
    s_lane = lax.broadcasted_iota(jnp.int32, (sources, sources * heads), 1)
    flat = jnp.sum(jnp.where(s_lane // heads == s_sub, weight, 0.0), axis=0, keepdims=True)
    mix = jnp.where(lane % heads == sub, jnp.broadcast_to(flat, (heads, rows)), 0.0)
    high = mix.astype(BF16)
    low = (mix - high.astype(F32)).astype(BF16)
    both = jnp.dot(
        jnp.concatenate([high, low], axis=0),
        got_out[...].reshape(sources * heads, DH),
        preferred_element_type=F32,
    )
    half_out[...] = (both[:heads] + both[heads:]).astype(BF16)
    half_lse[...] = peak + jnp.log(norm)

    pl.semaphore_wait(far_sem, 2)
    b_slot = lax.div(z, half) * batch + lax.rem(z, half) * n_c + c
    all_out[b_slot] = half_out[...]
    all_lse[pl.ds(b_slot, 1), :] = half_lse[...]
    b_copies = []
    order = sorted(range(-half + 1, half + 1), key=lambda d: -abs(d))
    for dz in order:
        for j in range(n_c):
            if dz == 0 and j == 0:
                continue
            index = (dz + half - 1) * n_c + j
            for k, (src, dst) in enumerate(
                ((half_out, all_out.at[b_slot]), (half_lse, all_lse.at[pl.ds(b_slot, 1), :]))
            ):
                copy = pltpu.make_async_remote_copy(
                    src_ref=src,
                    dst_ref=dst,
                    send_sem=b_send.at[index, k],
                    recv_sem=b_recv.at[index, k],
                    device_id={"seq": ring(dz), "sub": core(j)},
                    device_id_type=MESH,
                )
                copy.start()
                b_copies.append(copy)
    w_load.wait()
    for copy in b_copies:
        copy.wait_recv()

    l_one, l_two = all_lse[:batch, :], all_lse[batch:, :]
    peak = jnp.maximum(l_one, l_two)
    w_one, w_two = jnp.exp(l_one - peak), jnp.exp(l_two - peak)
    inv = 1.0 / (w_one + w_two)
    spot = lax.broadcasted_iota(jnp.int32, (batch, heads, rows), 0) * heads
    spot = spot + lax.broadcasted_iota(jnp.int32, (batch, heads, rows), 1)
    here = lax.broadcasted_iota(jnp.int32, (batch, heads, rows), 2) == spot
    blocks = []
    for weight in (w_one * inv, w_two * inv):
        expanded = jnp.broadcast_to(weight[:, None, :], (batch, heads, rows))
        blocks.append(jnp.where(here, expanded, 0.0).reshape(rows, rows))
    mix = jnp.concatenate(blocks, axis=1)
    high = mix.astype(BF16)
    low = (mix - high.astype(F32)).astype(BF16)
    parts = all_out[...].reshape(2 * rows, DH)
    att_rows[...] = jnp.dot(high, parts, preferred_element_type=F32) + jnp.dot(
        low, parts, preferred_element_type=F32
    )
    attention = jnp.concatenate(
        [att_rows[pl.ds(h, batch, stride=heads), :] for h in range(heads)], axis=1
    ).astype(BF16)
    projected = jnp.dot(attention, w_ref[...], preferred_element_type=F32)
    proj_mine[...] = projected.astype(BF16)
    proj_all[x] = proj_mine[...]

    c_copies = []
    for dx in sorted(range(1, n_x), key=lambda d: -min(d, n_x - d)):
        copy = pltpu.make_async_remote_copy(
            src_ref=proj_mine,
            dst_ref=proj_all.at[x],
            send_sem=c_send.at[dx - 1],
            recv_sem=c_recv.at[dx - 1],
            device_id={"head": lax.rem(x + dx, n_x)},
            device_id_type=MESH,
        )
        copy.start()
        c_copies.append(copy)
    for copy in c_copies:
        copy.wait_recv()
    summed = proj_all[0].astype(F32)
    for i in range(1, n_x):
        summed = summed + proj_all[i].astype(F32)
    out_ref[...] = summed.astype(out_ref.dtype)
    for copy in a_copies + b_copies + c_copies:
        copy.wait_send()


def on_device(sizes, queries, key_cache, value_cache, seq_lengths, slot_owner, slot_page, out_weight):
    n_z, n_x, n_c = sizes
    batch, heads = queries.shape[0], queries.shape[1] // DH
    slots = key_cache.shape[0]
    rows = batch * heads
    width = out_weight.shape[1]
    sources = n_z // 2 * n_c
    assert key_cache.shape[2] == DH and sources == batch and rows == DH
    vmem = pl.BlockSpec(memory_space=pltpu.VMEM)
    smem = pl.BlockSpec(memory_space=pltpu.SMEM)
    hbm = pl.BlockSpec(memory_space=pltpu.HBM)
    dma = pltpu.SemaphoreType.DMA
    return pl.pallas_call(
        functools.partial(kernel, sizes),
        out_shape=jax.ShapeDtypeStruct((batch, width), BF16),
        in_specs=[smem, smem, smem, vmem, vmem, hbm, hbm, hbm],
        out_specs=vmem,
        scratch_shapes=[
            pltpu.VMEM(key_cache.shape, BF16),
            pltpu.VMEM(value_cache.shape, BF16),
            pltpu.VMEM(out_weight.shape, BF16),
            pltpu.VMEM((rows, DH), F32),
            pltpu.VMEM((batch, heads, DH), F32),
            pltpu.VMEM((slots * heads, PAGE), F32),
            pltpu.VMEM((slots * heads, PAGE), F32),
            pltpu.VMEM((slots * heads, DH), BF16),
            pltpu.VMEM((rows, slots * heads), BF16),
            pltpu.VMEM((batch, heads, rows), F32),
            pltpu.VMEM((rows, rows), F32),
            pltpu.VMEM((batch, heads, DH), BF16),
            pltpu.VMEM((batch, 1, rows), F32),
            pltpu.VMEM((sources, heads, DH), BF16),
            pltpu.VMEM((sources, rows), F32),
            pltpu.VMEM((heads, DH), BF16),
            pltpu.VMEM((1, rows), F32),
            pltpu.VMEM((2 * batch, heads, DH), BF16),
            pltpu.VMEM((2 * batch, rows), F32),
            pltpu.VMEM((rows, DH), F32),
            pltpu.VMEM((batch, width), BF16),
            pltpu.VMEM((n_x, batch, width), BF16),
            dma((CHUNKS,)),
            dma((CHUNKS,)),
            dma,
            dma((sources, 2)),
            dma((sources, 2)),
            dma((n_z * n_c, 2)),
            dma((n_z * n_c, 2)),
            dma((n_x - 1,)),
            dma((n_x - 1,)),
            pltpu.SemaphoreType.REGULAR,
        ],
        compiler_params=pltpu.CompilerParams(collective_id=0, has_side_effects=True),
        name="decode",
    )(
        seq_lengths,
        slot_owner,
        slot_page,
        slot_owner.reshape(1, slots),
        queries,
        key_cache,
        value_cache,
        out_weight,
    )


def solution(mesh):
    sizes = (mesh.shape["seq"], mesh.shape["head"], mesh.shape["sub"])
    in_specs = (
        P("rep", "head"),
        P(("rep", "seq", "sub"), None, "head"),
        P(("rep", "seq", "sub"), None, "head"),
        P("rep"),
        P(("rep", "seq", "sub")),
        P(("rep", "seq", "sub")),
        P("head", ("seq", "sub")),
    )
    out_specs = P("rep", ("seq", "sub"))
    return jax.shard_map(
        functools.partial(on_device, sizes),
        mesh=mesh,
        in_specs=in_specs,
        out_specs=out_specs,
        check_vma=False,
    )
```

```python
import functools

import jax
import jax.numpy as jnp
from jax import lax
from jax.experimental import pallas as pl
from jax.experimental.pallas import tpu as pltpu
from jax.sharding import PartitionSpec as P

DH = 128
PAGE = 128
NEG = -1e30
CHUNKS = 4
F32 = jnp.float32
BF16 = jnp.bfloat16
MESH = pl.DeviceIdType.MESH


def kernel(
    sizes,
    lengths_hbm,
    owners_hbm,
    numbers_hbm,
    owner_row_hbm,
    q_hbm,
    k_hbm,
    v_hbm,
    w_hbm,
    out_ref,
    lengths,
    owners,
    numbers,
    owner_row,
    q_ref,
    k_ref,
    v_ref,
    w_ref,
    q_rows,
    q_seq,
    peaks,
    masses,
    hits,
    seq_lse,
    lse_diag,
    part_out,
    part_lse,
    got_out,
    got_lse,
    half_out,
    half_lse,
    all_out,
    all_lse,
    att_rows,
    proj_mine,
    proj_all,
    small_sem,
    k_sem,
    v_sem,
    w_sem,
    a_send,
    a_recv,
    b_send,
    b_recv,
    c_send,
    c_recv,
    far_sem,
):
    n_z, n_x, n_c = sizes
    batch, heads, slots = lengths.shape[0], q_ref.shape[1] // DH, owners.shape[0]
    half = n_z // 2
    near = half // 2
    z, x, c = lax.axis_index("seq"), lax.axis_index("head"), lax.axis_index("sub")
    rows = batch * heads
    per_chunk = slots // CHUNKS

    def ring(offset):
        return lax.rem(z + offset + n_z, n_z)

    def core(j):
        return lax.rem(c + j, n_c)

    small = [
        pltpu.make_async_copy(src, dst, small_sem.at[i])
        for i, (src, dst) in enumerate(
            (
                (owners_hbm, owners),
                (lengths_hbm, lengths),
                (numbers_hbm, numbers),
                (owner_row_hbm, owner_row),
                (q_hbm, q_ref),
            )
        )
    ]
    loads = []
    for hbm, ref, sem in ((k_hbm, k_ref, k_sem), (v_hbm, v_ref, v_sem)):
        copies = []
        for i in range(CHUNKS):
            span = pl.ds(i * per_chunk, per_chunk)
            copies.append(pltpu.make_async_copy(hbm.at[span], ref.at[span], sem.at[i]))
        loads.append(copies)
    w_load = pltpu.make_async_copy(w_hbm, w_ref, w_sem)
    for copy in small + loads[0]:
        copy.start()

    def wait_all(ref, count, sem):
        span = ref.at[pl.ds(0, count)]
        pltpu.make_async_copy(span, span, sem).wait()

    barrier = pltpu.get_barrier_semaphore()
    greeted = 0
    for dz in sorted(range(-near, near + 1), key=lambda d: -abs(d)):
        for j in range(n_c):
            if dz or j:
                greeted += 1
                pl.semaphore_signal(
                    barrier, inc=1, device_id={"seq": ring(dz), "sub": core(j)}, device_id_type=MESH
                )
    for dx in range(1, n_x):
        greeted += 1
        pl.semaphore_signal(
            barrier, inc=1, device_id={"head": lax.rem(x + dx, n_x)}, device_id_type=MESH
        )

    for copy in loads[1] + [w_load]:
        copy.start()
    for copy in small:
        copy.wait()

    lane = lax.broadcasted_iota(jnp.int32, (heads, rows), 1)
    sub = lax.broadcasted_iota(jnp.int32, (heads, rows), 0)
    diag = lane - sub

    for h in range(heads):
        q_rows[pl.ds(h, batch, stride=heads), :] = q_ref[:, h * DH : (h + 1) * DH].astype(F32)
    q_seq[...] = q_rows[...].reshape(batch, heads, DH)

    hit = (lax.broadcasted_iota(jnp.int32, (batch, slots), 0) == owner_row[...]).astype(BF16)
    spread_rows = lax.broadcasted_iota(jnp.int32, (slots, slots * heads), 0)
    spread_cols = lax.broadcasted_iota(jnp.int32, (slots, slots * heads), 1)
    spread = (spread_cols // heads == spread_rows).astype(BF16)
    wide = jnp.dot(hit, spread, preferred_element_type=F32)
    wide = jnp.broadcast_to(wide[:, None, :], (batch, heads, slots * heads))
    w_sub = lax.broadcasted_iota(jnp.int32, (batch, heads, slots * heads), 1)
    w_lane = lax.broadcasted_iota(jnp.int32, (batch, heads, slots * heads), 2)
    hits[...] = jnp.where(w_lane % heads == w_sub, wide, 0.0).reshape(rows, slots * heads).astype(BF16)

    scale = 1.0 / (float(DH) ** 0.5)
    pair_sub = lax.broadcasted_iota(jnp.int32, (2 * heads, PAGE), 0)
    pair_lane = lax.broadcasted_iota(jnp.int32, (2 * heads, PAGE), 1)
    first = pair_sub < heads

    probs = []
    top = jnp.full((heads, rows), NEG, F32)
    for i in range(CHUNKS):
        loads[0][i].wait()
        for pair in range(i * per_chunk // 2, (i + 1) * per_chunk // 2):
            a, b = 2 * pair, 2 * pair + 1
            own_a, own_b = owners[a], owners[b]
            q_pair = jnp.concatenate(
                [
                    q_seq[own_a],
                    q_seq[own_b],
                ],
                axis=0,
            ).astype(BF16)
            keys = k_ref[a : b + 1].reshape(2 * PAGE, DH)
            both = lax.dot_general(
                q_pair, keys, (((1,), (1,)), ((), ())), preferred_element_type=F32
            )
            scores = jnp.concatenate([both[:heads, :PAGE], both[heads:, PAGE:]], axis=0) * scale
            live_a = jnp.clip(lengths[own_a] - numbers[a] * PAGE, 0, PAGE)
            live_b = jnp.clip(lengths[own_b] - numbers[b] * PAGE, 0, PAGE)
            scores = jnp.where(pair_lane < jnp.where(first, live_a, live_b), scores, NEG)
            peak = jnp.max(scores, axis=1, keepdims=True)
            prob = jnp.exp(scores - peak).astype(BF16)
            mass = jnp.sum(prob.astype(F32), axis=1, keepdims=True)
            peak = jnp.broadcast_to(peak, (2 * heads, PAGE))
            mass = jnp.broadcast_to(mass, (2 * heads, PAGE))
            peaks[pl.ds(a * heads, 2 * heads), :] = peak
            masses[pl.ds(a * heads, 2 * heads), :] = mass
            probs.append(prob)
            top = jnp.maximum(top, jnp.where(diag == own_a * heads, peak[:heads], NEG))
            top = jnp.maximum(top, jnp.where(diag == own_b * heads, peak[heads:], NEG))

    def by_sequence(row_values):
        for b in range(batch):
            mine = jnp.max(
                jnp.where(lane // heads == b, row_values, 2 * NEG), axis=1, keepdims=True
            )
            seq_lse[b] = jnp.broadcast_to(mine, (heads, rows))

    by_sequence(top)
    total = jnp.zeros((heads, rows), F32)
    for s in range(slots):
        span = pl.ds(s * heads, heads)
        factor = jnp.exp(peaks[span, :] - seq_lse[owners[s]])
        total = total + jnp.where(diag == owners[s] * heads, factor * masses[span, :], 0.0)
    lse = jnp.where(total > 0.0, top + jnp.log(jnp.where(total > 0.0, total, 1.0)), NEG)
    by_sequence(lse)

    for b in range(batch):
        lse_diag[pl.ds(b * heads, heads), :] = jnp.where(lane % heads == sub, seq_lse[b], 0.0)
    tiled = lse_diag[pl.ds(0, batch, stride=heads), :]
    for h in range(1, heads):
        tiled = tiled + lse_diag[pl.ds(h, batch, stride=heads), :]
    part_lse[...] = tiled.reshape(batch, 1, rows)

    mine = jnp.zeros((rows, DH), F32)
    for i in range(CHUNKS):
        loads[1][i].wait()
        high, low = [], []
        for pair in range(i * per_chunk // 2, (i + 1) * per_chunk // 2):
            a, b = 2 * pair, 2 * pair + 1
            prob = probs[pair]
            block = jnp.concatenate(
                [
                    jnp.where(first, prob, jnp.zeros_like(prob)),
                    jnp.where(first, jnp.zeros_like(prob), prob),
                ],
                axis=1,
            )
            values = v_ref[a : b + 1].reshape(2 * PAGE, DH)
            page_out = jnp.dot(block, values, preferred_element_type=F32)
            span = pl.ds(a * heads, 2 * heads)
            level = jnp.concatenate([seq_lse[owners[a]], seq_lse[owners[b]]], axis=0)
            factor = jnp.exp(peaks[span, :] - level)
            page_out = page_out * factor
            high.append(page_out.astype(BF16))
            low.append((page_out - high[-1].astype(F32)).astype(BF16))
        hit = hits[:, i * per_chunk * heads : (i + 1) * per_chunk * heads]
        mine = mine + jnp.dot(
            jnp.concatenate([hit, hit], axis=1),
            jnp.concatenate(high + low, axis=0),
            preferred_element_type=F32,
        )
    part_out[...] = mine.astype(BF16).reshape(batch, heads, DH)

    pl.semaphore_wait(barrier, greeted)
    a_count = 0
    order = sorted(range(-near, near), key=lambda d: -abs(d))
    for dz in order:
        for j in range(n_c):
            target = lax.rem(ring(dz), half) * n_c + core(j)
            slot = (near - 1 - dz) * n_c + j
            if dz == 0 and j == 0:
                got_out[slot] = part_out[target]
                got_lse[pl.ds(slot, 1), :] = part_lse[target]
                continue
            for k, (src, dst) in enumerate(
                ((part_out.at[target], got_out.at[slot]), (part_lse.at[target], got_lse.at[pl.ds(slot, 1), :]))
            ):
                copy = pltpu.make_async_remote_copy(
                    src_ref=src,
                    dst_ref=dst,
                    send_sem=a_send.at[k],
                    recv_sem=a_recv.at[k],
                    device_id={"seq": ring(dz), "sub": core(j)},
                    device_id_type=MESH,
                )
                copy.start()
            a_count += 1
    for dz in (-near, near):
        pl.semaphore_signal(far_sem, inc=1, device_id={"seq": ring(dz)}, device_id_type=MESH)
    wait_all(got_lse, a_count, a_recv.at[1])
    wait_all(got_out, a_count, a_recv.at[0])

    sources = half * n_c
    levels = got_lse[...]
    peak = jnp.max(levels, axis=0, keepdims=True)
    weight = jnp.exp(levels - peak)
    norm = jnp.sum(weight, axis=0, keepdims=True)
    weight = weight / norm
    s_sub = lax.broadcasted_iota(jnp.int32, (sources, sources * heads), 0)
    s_lane = lax.broadcasted_iota(jnp.int32, (sources, sources * heads), 1)
    flat = jnp.sum(jnp.where(s_lane // heads == s_sub, weight, 0.0), axis=0, keepdims=True)
    mix = jnp.where(lane % heads == sub, jnp.broadcast_to(flat, (heads, rows)), 0.0)
    high = mix.astype(BF16)
    low = (mix - high.astype(F32)).astype(BF16)
    both = jnp.dot(
        jnp.concatenate([high, low], axis=0),
        got_out[...].reshape(sources * heads, DH),
        preferred_element_type=F32,
    )
    half_out[...] = (both[:heads] + both[heads:]).astype(BF16)
    half_lse[...] = peak + jnp.log(norm)

    pl.semaphore_wait(far_sem, 2)
    b_slot = lax.div(z, half) * batch + lax.rem(z, half) * n_c + c
    all_out[b_slot] = half_out[...]
    all_lse[pl.ds(b_slot, 1), :] = half_lse[...]
    b_count = 0
    order = sorted(range(-half + 1, half + 1), key=lambda d: -abs(d))
    for dz in order:
        for j in range(n_c):
            if dz == 0 and j == 0:
                continue
            for k, (src, dst) in enumerate(
                ((half_out, all_out.at[b_slot]), (half_lse, all_lse.at[pl.ds(b_slot, 1), :]))
            ):
                copy = pltpu.make_async_remote_copy(
                    src_ref=src,
                    dst_ref=dst,
                    send_sem=b_send.at[k],
                    recv_sem=b_recv.at[k],
                    device_id={"seq": ring(dz), "sub": core(j)},
                    device_id_type=MESH,
                )
                copy.start()
            b_count += 1
    w_load.wait()
    wait_all(part_lse, a_count, a_send.at[1])
    wait_all(part_out, a_count, a_send.at[0])
    wait_all(all_lse, b_count, b_recv.at[1])
    wait_all(all_out, b_count, b_recv.at[0])

    l_one, l_two = all_lse[:batch, :], all_lse[batch:, :]
    peak = jnp.maximum(l_one, l_two)
    w_one, w_two = jnp.exp(l_one - peak), jnp.exp(l_two - peak)
    inv = 1.0 / (w_one + w_two)
    spot = lax.broadcasted_iota(jnp.int32, (batch, heads, rows), 0) * heads
    spot = spot + lax.broadcasted_iota(jnp.int32, (batch, heads, rows), 1)
    here = lax.broadcasted_iota(jnp.int32, (batch, heads, rows), 2) == spot
    blocks = []
    for weight in (w_one * inv, w_two * inv):
        expanded = jnp.broadcast_to(weight[:, None, :], (batch, heads, rows))
        blocks.append(jnp.where(here, expanded, 0.0).reshape(rows, rows))
    mix = jnp.concatenate(blocks, axis=1)
    high = mix.astype(BF16)
    low = (mix - high.astype(F32)).astype(BF16)
    parts = all_out[...].reshape(2 * rows, DH)
    att_rows[...] = jnp.dot(high, parts, preferred_element_type=F32) + jnp.dot(
        low, parts, preferred_element_type=F32
    )
    attention = jnp.concatenate(
        [att_rows[pl.ds(h, batch, stride=heads), :] for h in range(heads)], axis=1
    ).astype(BF16)
    projected = jnp.dot(attention, w_ref[...], preferred_element_type=F32)
    proj_mine[...] = projected.astype(BF16)
    proj_all[x] = proj_mine[...]

    for dx in sorted(range(1, n_x), key=lambda d: -min(d, n_x - d)):
        copy = pltpu.make_async_remote_copy(
            src_ref=proj_mine,
            dst_ref=proj_all.at[x],
            send_sem=c_send,
            recv_sem=c_recv,
            device_id={"head": lax.rem(x + dx, n_x)},
            device_id_type=MESH,
        )
        copy.start()
    wait_all(all_lse, b_count, b_send.at[1])
    wait_all(all_out, b_count, b_send.at[0])
    wait_all(proj_all, n_x - 1, c_send)
    wait_all(proj_all, n_x - 1, c_recv)
    summed = proj_all[0].astype(F32)
    for i in range(1, n_x):
        summed = summed + proj_all[i].astype(F32)
    out_ref[...] = summed.astype(out_ref.dtype)


def on_device(sizes, queries, key_cache, value_cache, seq_lengths, slot_owner, slot_page, out_weight):
    n_z, n_x, n_c = sizes
    batch, heads = queries.shape[0], queries.shape[1] // DH
    slots = key_cache.shape[0]
    rows = batch * heads
    width = out_weight.shape[1]
    sources = n_z // 2 * n_c
    assert key_cache.shape[2] == DH and sources == batch and rows == DH
    hbm = pl.BlockSpec(memory_space=pltpu.HBM)
    dma = pltpu.SemaphoreType.DMA
    return pl.pallas_call(
        functools.partial(kernel, sizes),
        out_shape=pltpu.VMEM((batch, width), BF16),
        in_specs=[hbm] * 8,
        out_specs=pl.BlockSpec(memory_space=pltpu.VMEM),
        scratch_shapes=[
            pltpu.SMEM((batch,), jnp.int32),
            pltpu.SMEM((slots,), jnp.int32),
            pltpu.SMEM((slots,), jnp.int32),
            pltpu.VMEM((1, slots), jnp.int32),
            pltpu.VMEM(queries.shape, BF16),
            pltpu.VMEM(key_cache.shape, BF16),
            pltpu.VMEM(value_cache.shape, BF16),
            pltpu.VMEM(out_weight.shape, BF16),
            pltpu.VMEM((rows, DH), F32),
            pltpu.VMEM((batch, heads, DH), F32),
            pltpu.VMEM((slots * heads, PAGE), F32),
            pltpu.VMEM((slots * heads, PAGE), F32),
            pltpu.VMEM((rows, slots * heads), BF16),
            pltpu.VMEM((batch, heads, rows), F32),
            pltpu.VMEM((rows, rows), F32),
            pltpu.VMEM((batch, heads, DH), BF16),
            pltpu.VMEM((batch, 1, rows), F32),
            pltpu.VMEM((sources, heads, DH), BF16),
            pltpu.VMEM((sources, rows), F32),
            pltpu.VMEM((heads, DH), BF16),
            pltpu.VMEM((1, rows), F32),
            pltpu.VMEM((2 * batch, heads, DH), BF16),
            pltpu.VMEM((2 * batch, rows), F32),
            pltpu.VMEM((rows, DH), F32),
            pltpu.VMEM((batch, width), BF16),
            pltpu.VMEM((n_x, batch, width), BF16),
            dma((5,)),
            dma((CHUNKS,)),
            dma((CHUNKS,)),
            dma,
            dma((2,)),
            dma((2,)),
            dma((2,)),
            dma((2,)),
            dma,
            dma,
            pltpu.SemaphoreType.REGULAR,
        ],
        compiler_params=pltpu.CompilerParams(collective_id=0, has_side_effects=True),
        name="decode",
    )(
        seq_lengths,
        slot_owner,
        slot_page,
        slot_owner.reshape(1, slots),
        queries,
        key_cache,
        value_cache,
        out_weight,
    )


def solution(mesh):
    sizes = (mesh.shape["seq"], mesh.shape["head"], mesh.shape["sub"])
    in_specs = (
        P("rep", "head"),
        P(("rep", "seq", "sub"), None, "head"),
        P(("rep", "seq", "sub"), None, "head"),
        P("rep"),
        P(("rep", "seq", "sub")),
        P(("rep", "seq", "sub")),
        P("head", ("seq", "sub")),
    )
    out_specs = P("rep", ("seq", "sub"))
    return jax.shard_map(
        functools.partial(on_device, sizes),
        mesh=mesh,
        in_specs=in_specs,
        out_specs=out_specs,
        check_vma=False,
    )
```

```python
import functools

import jax
import jax.numpy as jnp
from jax import lax
from jax.experimental import pallas as pl
from jax.experimental.pallas import tpu as pltpu
from jax.sharding import PartitionSpec as P

DH = 128
PAGE = 128
NEG = -1e30
COPIES = 2
F32 = jnp.float32
BF16 = jnp.bfloat16
MESH = pl.DeviceIdType.MESH


def kernel(
    sizes,
    lengths_hbm,
    owners_hbm,
    numbers_hbm,
    owner_row_hbm,
    q_hbm,
    k_hbm,
    v_hbm,
    w_hbm,
    out_ref,
    lengths,
    owners,
    numbers,
    owner_row,
    q_ref,
    k_ref,
    v_ref,
    w_ref,
    q_rows,
    q_seq,
    peaks,
    masses,
    hits,
    seq_lse,
    lse_diag,
    part_out,
    part_lse,
    got_out,
    got_lse,
    own_out,
    own_lse,
    all_out,
    all_lse,
    att_rows,
    proj_mine,
    proj_all,
    small_sem,
    k_sem,
    v_sem,
    w_sem,
    a_send,
    a_recv,
    b_send,
    b_recv,
    c_send,
    c_recv,
    far_sem,
    side_sem,
):
    n_z, n_x, n_c = sizes
    batch, heads, slots = lengths.shape[0], q_ref.shape[1] // DH, owners.shape[0]
    half = n_z // 2
    near = half // 2
    seg = n_z // COPIES
    per = batch // (seg * n_c)
    sources = seg * n_c
    z, x, c = lax.axis_index("seq"), lax.axis_index("head"), lax.axis_index("sub")
    rows = batch * heads

    def ring(offset):
        return lax.rem(z + offset + n_z, n_z)

    def core(j):
        return lax.rem(c + j, n_c)

    small = [
        pltpu.make_async_copy(src, dst, small_sem.at[i])
        for i, (src, dst) in enumerate(
            (
                (owners_hbm, owners),
                (lengths_hbm, lengths),
                (numbers_hbm, numbers),
                (owner_row_hbm, owner_row),
                (q_hbm, q_ref),
            )
        )
    ]
    k_load = pltpu.make_async_copy(k_hbm, k_ref, k_sem)
    v_load = pltpu.make_async_copy(v_hbm, v_ref, v_sem)
    w_load = pltpu.make_async_copy(w_hbm, w_ref, w_sem)
    for copy in small + [k_load, v_load, w_load]:
        copy.start()

    def wait_all(ref, count, sem):
        span = ref.at[pl.ds(0, count)]
        pltpu.make_async_copy(span, span, sem).wait()

    barrier = pltpu.get_barrier_semaphore()
    greeted = 0
    for dz in sorted(range(-near, near + 1), key=lambda d: -abs(d)):
        for j in range(n_c):
            if dz or j:
                greeted += 1
                pl.semaphore_signal(
                    barrier, inc=1, device_id={"seq": ring(dz), "sub": core(j)}, device_id_type=MESH
                )
    for dx in (1, n_x - 1):
        greeted += 1
        pl.semaphore_signal(
            barrier, inc=1, device_id={"head": lax.rem(x + dx, n_x)}, device_id_type=MESH
        )

    for copy in small:
        copy.wait()

    lane = lax.broadcasted_iota(jnp.int32, (heads, rows), 1)
    sub = lax.broadcasted_iota(jnp.int32, (heads, rows), 0)
    diag = lane - sub

    for h in range(heads):
        q_rows[pl.ds(h, batch, stride=heads), :] = q_ref[:, h * DH : (h + 1) * DH].astype(F32)
    q_seq[...] = q_rows[...].reshape(batch, heads, DH)

    hit = (lax.broadcasted_iota(jnp.int32, (batch, slots), 0) == owner_row[...]).astype(BF16)
    spread_rows = lax.broadcasted_iota(jnp.int32, (slots, slots * heads), 0)
    spread_cols = lax.broadcasted_iota(jnp.int32, (slots, slots * heads), 1)
    spread = (spread_cols // heads == spread_rows).astype(BF16)
    wide = jnp.dot(hit, spread, preferred_element_type=F32)
    wide = jnp.broadcast_to(wide[:, None, :], (batch, heads, slots * heads))
    w_sub = lax.broadcasted_iota(jnp.int32, (batch, heads, slots * heads), 1)
    w_lane = lax.broadcasted_iota(jnp.int32, (batch, heads, slots * heads), 2)
    hits[...] = jnp.where(w_lane % heads == w_sub, wide, 0.0).reshape(rows, slots * heads).astype(BF16)

    scale = 1.0 / (float(DH) ** 0.5)
    pair_sub = lax.broadcasted_iota(jnp.int32, (2 * heads, PAGE), 0)
    pair_lane = lax.broadcasted_iota(jnp.int32, (2 * heads, PAGE), 1)
    first = pair_sub < heads

    probs = []
    top = jnp.full((heads, rows), NEG, F32)
    k_load.wait()
    for pair in range(slots // 2):
        a, b = 2 * pair, 2 * pair + 1
        own_a, own_b = owners[a], owners[b]
        q_pair = jnp.concatenate(
            [
                q_seq[own_a],
                q_seq[own_b],
            ],
            axis=0,
        ).astype(BF16)
        keys = k_ref[a : b + 1].reshape(2 * PAGE, DH)
        both = lax.dot_general(
            q_pair, keys, (((1,), (1,)), ((), ())), preferred_element_type=F32
        )
        scores = jnp.concatenate([both[:heads, :PAGE], both[heads:, PAGE:]], axis=0) * scale
        live_a = jnp.clip(lengths[own_a] - numbers[a] * PAGE, 0, PAGE)
        live_b = jnp.clip(lengths[own_b] - numbers[b] * PAGE, 0, PAGE)
        scores = jnp.where(pair_lane < jnp.where(first, live_a, live_b), scores, NEG)
        peak = jnp.max(scores, axis=1, keepdims=True)
        prob = jnp.exp(scores - peak).astype(BF16)
        mass = jnp.sum(prob.astype(F32), axis=1, keepdims=True)
        peak = jnp.broadcast_to(peak, (2 * heads, PAGE))
        mass = jnp.broadcast_to(mass, (2 * heads, PAGE))
        peaks[pl.ds(a * heads, 2 * heads), :] = peak
        masses[pl.ds(a * heads, 2 * heads), :] = mass
        probs.append(prob)
        top = jnp.maximum(top, jnp.where(diag == own_a * heads, peak[:heads], NEG))
        top = jnp.maximum(top, jnp.where(diag == own_b * heads, peak[heads:], NEG))

    v_load.wait()

    def by_sequence(row_values):
        for b in range(batch):
            mine = jnp.max(
                jnp.where(lane // heads == b, row_values, 2 * NEG), axis=1, keepdims=True
            )
            seq_lse[b] = jnp.broadcast_to(mine, (heads, rows))

    by_sequence(top)
    total = jnp.zeros((heads, rows), F32)
    for s in range(slots):
        span = pl.ds(s * heads, heads)
        factor = jnp.exp(peaks[span, :] - seq_lse[owners[s]])
        total = total + jnp.where(diag == owners[s] * heads, factor * masses[span, :], 0.0)
    lse = jnp.where(total > 0.0, top + jnp.log(jnp.where(total > 0.0, total, 1.0)), NEG)
    by_sequence(lse)

    for b in range(batch):
        lse_diag[pl.ds(b * heads, heads), :] = jnp.where(lane % heads == sub, seq_lse[b], 0.0)
    tiled = lse_diag[pl.ds(0, batch, stride=heads), :]
    for h in range(1, heads):
        tiled = tiled + lse_diag[pl.ds(h, batch, stride=heads), :]
    part_lse[...] = tiled

    high, low = [], []
    for pair in range(slots // 2):
        a, b = 2 * pair, 2 * pair + 1
        prob = probs[pair]
        block = jnp.concatenate(
            [
                jnp.where(first, prob, jnp.zeros_like(prob)),
                jnp.where(first, jnp.zeros_like(prob), prob),
            ],
            axis=1,
        )
        values = v_ref[a : b + 1].reshape(2 * PAGE, DH)
        page_out = jnp.dot(block, values, preferred_element_type=F32)
        span = pl.ds(a * heads, 2 * heads)
        level = jnp.concatenate([seq_lse[owners[a]], seq_lse[owners[b]]], axis=0)
        factor = jnp.exp(peaks[span, :] - level)
        page_out = page_out * factor
        high.append(page_out.astype(BF16))
        low.append((page_out - high[-1].astype(F32)).astype(BF16))
    hit = hits[...]
    mine = jnp.dot(hit, jnp.concatenate(high, axis=0), preferred_element_type=F32)
    mine = mine + jnp.dot(hit, jnp.concatenate(low, axis=0), preferred_element_type=F32)
    part_out[...] = mine.astype(BF16).reshape(batch // per, per, heads, DH)

    pl.semaphore_wait(barrier, greeted)
    a_count = 0
    for dz in sorted(range(-(seg // 2), seg // 2), key=lambda d: -abs(d)):
        for j in range(n_c):
            target = lax.rem(ring(dz), seg) * n_c + core(j)
            slot = (seg // 2 - 1 - dz) * n_c + j
            src_rows, dst_rows = pl.ds(target * per, per), pl.ds(slot * per, per)
            if dz == 0 and j == 0:
                got_out[slot] = part_out[target]
                got_lse[dst_rows, :] = part_lse[src_rows, :]
                continue
            for k, (src, dst) in enumerate(
                (
                    (part_out.at[target], got_out.at[slot]),
                    (part_lse.at[src_rows, :], got_lse.at[dst_rows, :]),
                )
            ):
                copy = pltpu.make_async_remote_copy(
                    src_ref=src,
                    dst_ref=dst,
                    send_sem=a_send.at[k],
                    recv_sem=a_recv.at[k],
                    device_id={"seq": ring(dz), "sub": core(j)},
                    device_id_type=MESH,
                )
                copy.start()
            a_count += 1
    for dz in (-near, near):
        pl.semaphore_signal(far_sem, inc=1, device_id={"seq": ring(dz)}, device_id_type=MESH)
    for dx in (1, n_x - 1):
        pl.semaphore_signal(
            side_sem.at[0], inc=1, device_id={"head": lax.rem(x + dx, n_x)}, device_id_type=MESH
        )
    wait_all(got_lse, a_count * per, a_recv.at[1])
    wait_all(got_out, a_count, a_recv.at[0])

    s_sub = lax.broadcasted_iota(jnp.int32, (sources, rows), 0)
    s_lane = lax.broadcasted_iota(jnp.int32, (sources, rows), 1)
    mixes = []
    for i in range(per):
        levels = got_lse[pl.ds(i, sources, stride=per), :]
        peak = jnp.max(levels, axis=0, keepdims=True)
        weight = jnp.exp(levels - peak)
        norm = jnp.sum(weight, axis=0, keepdims=True)
        weight = weight / norm
        flat = jnp.sum(
            jnp.where(s_lane // heads == s_sub * per + i, weight, 0.0), axis=0, keepdims=True
        )
        mixes.append(jnp.where(lane % heads == sub, jnp.broadcast_to(flat, (heads, rows)), 0.0))
        own_lse[pl.ds(i, 1), :] = peak + jnp.log(norm)
    mix = jnp.concatenate(mixes, axis=0)
    high = mix.astype(BF16)
    low = (mix - high.astype(F32)).astype(BF16)
    parts = got_out[...].reshape(rows, DH)
    own = jnp.dot(high, parts, preferred_element_type=F32) + jnp.dot(
        low, parts, preferred_element_type=F32
    )
    own_out[...] = own.astype(BF16).reshape(per, heads, DH)

    pl.semaphore_wait(far_sem, 2)
    b_slot = lax.div(z, seg) * (batch // per) + lax.rem(z, seg) * n_c + c
    b_rows = pl.ds(b_slot * per, per)
    all_out[b_slot] = own_out[...]
    all_lse[b_rows, :] = own_lse[...]
    b_count = 0
    order = sorted(range(-half + 1, half + 1), key=lambda d: -abs(d))
    for dz in order:
        for j in range(n_c):
            if dz == 0 and j == 0:
                continue
            for k, (src, dst) in enumerate(
                ((own_out, all_out.at[b_slot]), (own_lse, all_lse.at[b_rows, :]))
            ):
                copy = pltpu.make_async_remote_copy(
                    src_ref=src,
                    dst_ref=dst,
                    send_sem=b_send.at[k],
                    recv_sem=b_recv.at[k],
                    device_id={"seq": ring(dz), "sub": core(j)},
                    device_id_type=MESH,
                )
                copy.start()
            b_count += 1
    pl.semaphore_wait(side_sem.at[0], 2)
    for dx in (2, n_x - 2):
        pl.semaphore_signal(
            side_sem.at[1], inc=1, device_id={"head": lax.rem(x + dx, n_x)}, device_id_type=MESH
        )
    w_load.wait()
    wait_all(part_lse, a_count * per, a_send.at[1])
    wait_all(part_out, a_count, a_send.at[0])
    wait_all(all_lse, b_count * per, b_recv.at[1])
    wait_all(all_out, b_count, b_recv.at[0])

    levels = [all_lse[i * batch : (i + 1) * batch, :] for i in range(COPIES)]
    peak = functools.reduce(jnp.maximum, levels)
    weights = [jnp.exp(level - peak) for level in levels]
    inv = 1.0 / sum(weights)
    spot = lax.broadcasted_iota(jnp.int32, (batch, heads, rows), 0) * heads
    spot = spot + lax.broadcasted_iota(jnp.int32, (batch, heads, rows), 1)
    here = lax.broadcasted_iota(jnp.int32, (batch, heads, rows), 2) == spot
    blocks = []
    for weight in weights:
        expanded = jnp.broadcast_to((weight * inv)[:, None, :], (batch, heads, rows))
        blocks.append(jnp.where(here, expanded, 0.0).reshape(rows, rows))
    mix = jnp.concatenate(blocks, axis=1)
    high = mix.astype(BF16)
    low = (mix - high.astype(F32)).astype(BF16)
    parts = all_out[...].reshape(COPIES * rows, DH)
    att_rows[...] = jnp.dot(high, parts, preferred_element_type=F32) + jnp.dot(
        low, parts, preferred_element_type=F32
    )
    attention = jnp.concatenate(
        [att_rows[pl.ds(h, batch, stride=heads), :] for h in range(heads)], axis=1
    ).astype(BF16)
    projected = jnp.dot(attention, w_ref[...], preferred_element_type=F32)
    proj_mine[...] = projected.astype(BF16)
    proj_all[x] = proj_mine[...]

    pl.semaphore_wait(side_sem.at[1], 2)
    for dx in sorted(range(1, n_x), key=lambda d: -min(d, n_x - d)):
        copy = pltpu.make_async_remote_copy(
            src_ref=proj_mine,
            dst_ref=proj_all.at[x],
            send_sem=c_send,
            recv_sem=c_recv,
            device_id={"head": lax.rem(x + dx, n_x)},
            device_id_type=MESH,
        )
        copy.start()
    wait_all(all_lse, b_count * per, b_send.at[1])
    wait_all(all_out, b_count, b_send.at[0])
    wait_all(proj_all, n_x - 1, c_send)
    wait_all(proj_all, n_x - 1, c_recv)
    summed = proj_all[0].astype(F32)
    for i in range(1, n_x):
        summed = summed + proj_all[i].astype(F32)
    out_ref[...] = summed.astype(out_ref.dtype)


def on_device(sizes, queries, key_cache, value_cache, seq_lengths, slot_owner, slot_page, out_weight):
    n_z, n_x, n_c = sizes
    batch, heads = queries.shape[0], queries.shape[1] // DH
    slots = key_cache.shape[0]
    rows = batch * heads
    width = out_weight.shape[1]
    sources = n_z // COPIES * n_c
    per = batch // sources
    assert key_cache.shape[2] == DH and sources * per == batch and rows == DH
    hbm = pl.BlockSpec(memory_space=pltpu.HBM)
    dma = pltpu.SemaphoreType.DMA
    return pl.pallas_call(
        functools.partial(kernel, sizes),
        out_shape=pltpu.VMEM((batch, width), BF16),
        in_specs=[hbm] * 8,
        out_specs=pl.BlockSpec(memory_space=pltpu.VMEM),
        scratch_shapes=[
            pltpu.SMEM((batch,), jnp.int32),
            pltpu.SMEM((slots,), jnp.int32),
            pltpu.SMEM((slots,), jnp.int32),
            pltpu.VMEM((1, slots), jnp.int32),
            pltpu.VMEM(queries.shape, BF16),
            pltpu.VMEM(key_cache.shape, BF16),
            pltpu.VMEM(value_cache.shape, BF16),
            pltpu.VMEM(out_weight.shape, BF16),
            pltpu.VMEM((rows, DH), F32),
            pltpu.VMEM((batch, heads, DH), F32),
            pltpu.VMEM((slots * heads, PAGE), F32),
            pltpu.VMEM((slots * heads, PAGE), F32),
            pltpu.VMEM((rows, slots * heads), BF16),
            pltpu.VMEM((batch, heads, rows), F32),
            pltpu.VMEM((rows, rows), F32),
            pltpu.VMEM((batch // per, per, heads, DH), BF16),
            pltpu.VMEM((batch, rows), F32),
            pltpu.VMEM((sources, per, heads, DH), BF16),
            pltpu.VMEM((batch, rows), F32),
            pltpu.VMEM((per, heads, DH), BF16),
            pltpu.VMEM((per, rows), F32),
            pltpu.VMEM((COPIES * batch // per, per, heads, DH), BF16),
            pltpu.VMEM((COPIES * batch, rows), F32),
            pltpu.VMEM((rows, DH), F32),
            pltpu.VMEM((batch, width), BF16),
            pltpu.VMEM((n_x, batch, width), BF16),
            dma((5,)),
            dma,
            dma,
            dma,
            dma((2,)),
            dma((2,)),
            dma((2,)),
            dma((2,)),
            dma,
            dma,
            pltpu.SemaphoreType.REGULAR,
            pltpu.SemaphoreType.REGULAR((2,)),
        ],
        compiler_params=pltpu.CompilerParams(collective_id=0, has_side_effects=True),
        name="decode",
    )(
        seq_lengths,
        slot_owner,
        slot_page,
        slot_owner.reshape(1, slots),
        queries,
        key_cache,
        value_cache,
        out_weight,
    )


def solution(mesh):
    sizes = (mesh.shape["seq"], mesh.shape["head"], mesh.shape["sub"])
    in_specs = (
        P("rep", "head"),
        P(("rep", "seq", "sub"), None, "head"),
        P(("rep", "seq", "sub"), None, "head"),
        P("rep"),
        P(("rep", "seq", "sub")),
        P(("rep", "seq", "sub")),
        P("head", ("seq", "sub")),
    )
    out_specs = P("rep", ("seq", "sub"))
    return jax.shard_map(
        functools.partial(on_device, sizes),
        mesh=mesh,
        in_specs=in_specs,
        out_specs=out_specs,
        check_vma=False,
    )
```

```python
import functools

import jax
import jax.numpy as jnp
from jax import lax
from jax.experimental import pallas as pl
from jax.experimental.pallas import tpu as pltpu
from jax.sharding import PartitionSpec as P

DH = 128
PAGE = 128
NEG = -1e30
COPIES = 2
F32 = jnp.float32
BF16 = jnp.bfloat16
MESH = pl.DeviceIdType.MESH


def kernel(
    sizes,
    lengths_hbm,
    owners_hbm,
    numbers_hbm,
    owner_row_hbm,
    q_hbm,
    k_hbm,
    v_hbm,
    w_hbm,
    out_ref,
    lengths,
    owners,
    numbers,
    owner_row,
    q_ref,
    k_ref,
    v_ref,
    w_ref,
    q_rows,
    q_seq,
    peaks,
    masses,
    hits,
    seq_lse,
    lse_diag,
    part_out,
    part_lse,
    got_out,
    got_lse,
    own_out,
    own_lse,
    all_out,
    all_lse,
    att_rows,
    proj_mine,
    proj_all,
    small_sem,
    k_sem,
    v_sem,
    w_sem,
    w_pass,
    a_send,
    a_recv,
    b_send,
    b_recv,
    c_send,
    c_recv,
    far_sem,
    side_sem,
):
    n_z, n_x, n_c = sizes
    batch, heads, slots = lengths.shape[0], q_ref.shape[1] // DH, owners.shape[0]
    half = n_z // 2
    near = half // 2
    seg = n_z // COPIES
    per = batch // seg
    top = n_c - 1
    sources = seg * n_c
    z, x, c = lax.axis_index("seq"), lax.axis_index("head"), lax.axis_index("sub")
    rows = batch * heads

    def ring(offset):
        return lax.rem(z + offset + n_z, n_z)

    small = [
        pltpu.make_async_copy(src, dst, small_sem.at[i])
        for i, (src, dst) in enumerate(
            (
                (owners_hbm, owners),
                (lengths_hbm, lengths),
                (numbers_hbm, numbers),
                (owner_row_hbm, owner_row),
                (q_hbm, q_ref),
            )
        )
    ]
    k_load = pltpu.make_async_copy(k_hbm, k_ref, k_sem)
    v_load = pltpu.make_async_copy(v_hbm, v_ref, v_sem)
    w_load = pltpu.make_async_copy(w_hbm, w_ref.at[top], w_sem)
    for copy in small + [k_load, v_load]:
        copy.start()

    def wait_all(ref, count, sem):
        span = ref.at[pl.ds(0, count)]
        pltpu.make_async_copy(span, span, sem).wait()

    barrier = pltpu.get_barrier_semaphore()

    def greet(**where):
        pl.semaphore_signal(barrier, inc=1, device_id=where, device_id_type=MESH)

    @pl.when(c == top)
    def _():
        for dz in sorted(range(-near, near + 1), key=lambda d: -abs(d)):
            for core in range(n_c):
                if dz or core != top:
                    greet(seq=ring(dz), sub=core)
        for dx in (1, n_x - 1):
            greet(head=lax.rem(x + dx, n_x), sub=top)
        w_load.start()

    @pl.when(c != top)
    def _():
        for dx in (0, 1, n_x - 1):
            greet(head=lax.rem(x + dx, n_x), sub=top)

    greeted_top = 2 * near + (n_c - 1) + 2 * n_c
    greeted_other = 2 * near + 1

    for copy in small:
        copy.wait()

    lane = lax.broadcasted_iota(jnp.int32, (heads, rows), 1)
    sub = lax.broadcasted_iota(jnp.int32, (heads, rows), 0)
    diag = lane - sub

    for h in range(heads):
        q_rows[pl.ds(h, batch, stride=heads), :] = q_ref[:, h * DH : (h + 1) * DH].astype(F32)
    q_seq[...] = q_rows[...].reshape(batch, heads, DH)

    hit = (lax.broadcasted_iota(jnp.int32, (batch, slots), 0) == owner_row[...]).astype(BF16)
    spread_rows = lax.broadcasted_iota(jnp.int32, (slots, slots * heads), 0)
    spread_cols = lax.broadcasted_iota(jnp.int32, (slots, slots * heads), 1)
    spread = (spread_cols // heads == spread_rows).astype(BF16)
    wide = jnp.dot(hit, spread, preferred_element_type=F32)
    wide = jnp.broadcast_to(wide[:, None, :], (batch, heads, slots * heads))
    w_sub = lax.broadcasted_iota(jnp.int32, (batch, heads, slots * heads), 1)
    w_lane = lax.broadcasted_iota(jnp.int32, (batch, heads, slots * heads), 2)
    hits[...] = jnp.where(w_lane % heads == w_sub, wide, 0.0).reshape(rows, slots * heads).astype(BF16)

    scale = 1.0 / (float(DH) ** 0.5)
    pair_sub = lax.broadcasted_iota(jnp.int32, (2 * heads, PAGE), 0)
    pair_lane = lax.broadcasted_iota(jnp.int32, (2 * heads, PAGE), 1)
    first = pair_sub < heads

    probs = []
    peak_diag = jnp.full((heads, rows), NEG, F32)
    k_load.wait()
    for pair in range(slots // 2):
        a, b = 2 * pair, 2 * pair + 1
        own_a, own_b = owners[a], owners[b]
        q_pair = jnp.concatenate(
            [
                q_seq[own_a],
                q_seq[own_b],
            ],
            axis=0,
        ).astype(BF16)
        keys = k_ref[a : b + 1].reshape(2 * PAGE, DH)
        both = lax.dot_general(
            q_pair, keys, (((1,), (1,)), ((), ())), preferred_element_type=F32
        )
        scores = jnp.concatenate([both[:heads, :PAGE], both[heads:, PAGE:]], axis=0) * scale
        live_a = jnp.clip(lengths[own_a] - numbers[a] * PAGE, 0, PAGE)
        live_b = jnp.clip(lengths[own_b] - numbers[b] * PAGE, 0, PAGE)
        scores = jnp.where(pair_lane < jnp.where(first, live_a, live_b), scores, NEG)
        peak = jnp.max(scores, axis=1, keepdims=True)
        prob = jnp.exp(scores - peak).astype(BF16)
        mass = jnp.sum(prob.astype(F32), axis=1, keepdims=True)
        peak = jnp.broadcast_to(peak, (2 * heads, PAGE))
        mass = jnp.broadcast_to(mass, (2 * heads, PAGE))
        peaks[pl.ds(a * heads, 2 * heads), :] = peak
        masses[pl.ds(a * heads, 2 * heads), :] = mass
        probs.append(prob)
        peak_diag = jnp.maximum(peak_diag, jnp.where(diag == own_a * heads, peak[:heads], NEG))
        peak_diag = jnp.maximum(peak_diag, jnp.where(diag == own_b * heads, peak[heads:], NEG))

    v_load.wait()

    def by_sequence(row_values):
        for b in range(batch):
            mine = jnp.max(
                jnp.where(lane // heads == b, row_values, 2 * NEG), axis=1, keepdims=True
            )
            seq_lse[b] = jnp.broadcast_to(mine, (heads, rows))

    by_sequence(peak_diag)
    total = jnp.zeros((heads, rows), F32)
    for s in range(slots):
        span = pl.ds(s * heads, heads)
        factor = jnp.exp(peaks[span, :] - seq_lse[owners[s]])
        total = total + jnp.where(diag == owners[s] * heads, factor * masses[span, :], 0.0)
    lse = jnp.where(total > 0.0, peak_diag + jnp.log(jnp.where(total > 0.0, total, 1.0)), NEG)
    by_sequence(lse)

    for b in range(batch):
        lse_diag[pl.ds(b * heads, heads), :] = jnp.where(lane % heads == sub, seq_lse[b], 0.0)
    tiled = lse_diag[pl.ds(0, batch, stride=heads), :]
    for h in range(1, heads):
        tiled = tiled + lse_diag[pl.ds(h, batch, stride=heads), :]
    part_lse[...] = tiled

    high, low = [], []
    for pair in range(slots // 2):
        a, b = 2 * pair, 2 * pair + 1
        prob = probs[pair]
        block = jnp.concatenate(
            [
                jnp.where(first, prob, jnp.zeros_like(prob)),
                jnp.where(first, jnp.zeros_like(prob), prob),
            ],
            axis=1,
        )
        values = v_ref[a : b + 1].reshape(2 * PAGE, DH)
        page_out = jnp.dot(block, values, preferred_element_type=F32)
        span = pl.ds(a * heads, 2 * heads)
        level = jnp.concatenate([seq_lse[owners[a]], seq_lse[owners[b]]], axis=0)
        factor = jnp.exp(peaks[span, :] - level)
        page_out = page_out * factor
        high.append(page_out.astype(BF16))
        low.append((page_out - high[-1].astype(F32)).astype(BF16))
    hit = hits[...]
    mine = jnp.dot(hit, jnp.concatenate(high, axis=0), preferred_element_type=F32)
    mine = mine + jnp.dot(hit, jnp.concatenate(low, axis=0), preferred_element_type=F32)
    part_out[...] = mine.astype(BF16).reshape(seg, per, heads, DH)

    def send_parts(core):
        sent = 0
        for dz in sorted(range(-(seg // 2), seg // 2), key=lambda d: -abs(d)):
            target = lax.rem(ring(dz), seg)
            slot = (seg // 2 - 1 - dz) * n_c + core
            src_rows, dst_rows = pl.ds(target * per, per), pl.ds(slot * per, per)
            if dz == 0 and core == top:
                got_out[slot] = part_out[target]
                got_lse[dst_rows, :] = part_lse[src_rows, :]
                continue
            for k, (src, dst) in enumerate(
                (
                    (part_out.at[target], got_out.at[slot]),
                    (part_lse.at[src_rows, :], got_lse.at[dst_rows, :]),
                )
            ):
                pltpu.make_async_remote_copy(
                    src_ref=src,
                    dst_ref=dst,
                    send_sem=a_send.at[k],
                    recv_sem=a_recv.at[k],
                    device_id={"seq": ring(dz), "sub": top},
                    device_id_type=MESH,
                ).start()
            sent += 1
        return sent

    def other_core():
        pl.semaphore_wait(barrier, greeted_other)
        sent = send_parts(0)
        weights = pltpu.make_async_remote_copy(
            src_ref=w_hbm,
            dst_ref=w_ref.at[0],
            send_sem=w_pass.at[0],
            recv_sem=w_pass.at[1],
            device_id={"sub": top},
            device_id_type=MESH,
        )
        weights.start()
        wait_all(part_lse, sent * per, a_send.at[1])
        wait_all(part_out, sent, a_send.at[0])
        weights.wait_send()
        wait_all(proj_all, n_x, c_recv)

    def top_core():
        pl.semaphore_wait(barrier, greeted_top)
        sent = send_parts(top)
        for dz in (-near, near):
            pl.semaphore_signal(far_sem, inc=1, device_id={"seq": ring(dz)}, device_id_type=MESH)
        for dx in (1, n_x - 1):
            pl.semaphore_signal(
                side_sem.at[0], inc=1, device_id={"head": lax.rem(x + dx, n_x)}, device_id_type=MESH
            )
        wait_all(got_lse, (sources - 1) * per, a_recv.at[1])
        wait_all(got_out, sources - 1, a_recv.at[0])

        wide_rows = rows * n_c
        s_sub = lax.broadcasted_iota(jnp.int32, (sources, wide_rows), 0)
        s_lane = lax.broadcasted_iota(jnp.int32, (sources, wide_rows), 1)
        m_lane = lax.broadcasted_iota(jnp.int32, (heads, wide_rows), 1)
        m_sub = lax.broadcasted_iota(jnp.int32, (heads, wide_rows), 0)
        mixes = []
        for i in range(per):
            levels = got_lse[pl.ds(i, sources, stride=per), :]
            peak = jnp.max(levels, axis=0, keepdims=True)
            weight = jnp.exp(levels - peak)
            norm = jnp.sum(weight, axis=0, keepdims=True)
            weight = jnp.concatenate([weight / norm] * n_c, axis=1)
            flat = jnp.sum(
                jnp.where(s_lane // heads == s_sub * per + i, weight, 0.0), axis=0, keepdims=True
            )
            mixes.append(jnp.where(m_lane % heads == m_sub, jnp.broadcast_to(flat, (heads, wide_rows)), 0.0))
            own_lse[pl.ds(i, 1), :] = peak + jnp.log(norm)
        mix = jnp.concatenate(mixes, axis=0)
        high = mix.astype(BF16)
        low = (mix - high.astype(F32)).astype(BF16)
        parts = got_out[...].reshape(wide_rows, DH)
        own = jnp.dot(high, parts, preferred_element_type=F32) + jnp.dot(
            low, parts, preferred_element_type=F32
        )
        own_out[...] = own.astype(BF16).reshape(per, heads, DH)

        pl.semaphore_wait(far_sem, 2)
        b_rows = pl.ds(z * per, per)
        all_out[z] = own_out[...]
        all_lse[b_rows, :] = own_lse[...]
        for dz in sorted(range(-half + 1, half + 1), key=lambda d: -abs(d)):
            if dz == 0:
                continue
            for k, (src, dst) in enumerate(
                ((own_out, all_out.at[z]), (own_lse, all_lse.at[b_rows, :]))
            ):
                pltpu.make_async_remote_copy(
                    src_ref=src,
                    dst_ref=dst,
                    send_sem=b_send.at[k],
                    recv_sem=b_recv.at[k],
                    device_id={"seq": ring(dz)},
                    device_id_type=MESH,
                ).start()
        pl.semaphore_wait(side_sem.at[0], 2)
        for dx in (2, n_x - 2):
            pl.semaphore_signal(
                side_sem.at[1], inc=1, device_id={"head": lax.rem(x + dx, n_x)}, device_id_type=MESH
            )
        w_load.wait()
        pltpu.make_async_copy(w_ref.at[0], w_ref.at[0], w_pass.at[1]).wait()
        wait_all(part_lse, sent * per, a_send.at[1])
        wait_all(part_out, sent, a_send.at[0])
        wait_all(all_lse, (n_z - 1) * per, b_recv.at[1])
        wait_all(all_out, n_z - 1, b_recv.at[0])

        levels = [all_lse[i * batch : (i + 1) * batch, :] for i in range(COPIES)]
        peak = functools.reduce(jnp.maximum, levels)
        weights = [jnp.exp(level - peak) for level in levels]
        inv = 1.0 / sum(weights)
        spot = lax.broadcasted_iota(jnp.int32, (batch, heads, rows), 0) * heads
        spot = spot + lax.broadcasted_iota(jnp.int32, (batch, heads, rows), 1)
        here = lax.broadcasted_iota(jnp.int32, (batch, heads, rows), 2) == spot
        blocks = []
        for weight in weights:
            expanded = jnp.broadcast_to((weight * inv)[:, None, :], (batch, heads, rows))
            blocks.append(jnp.where(here, expanded, 0.0).reshape(rows, rows))
        mix = jnp.concatenate(blocks, axis=1)
        high = mix.astype(BF16)
        low = (mix - high.astype(F32)).astype(BF16)
        parts = all_out[...].reshape(COPIES * rows, DH)
        att_rows[...] = jnp.dot(high, parts, preferred_element_type=F32) + jnp.dot(
            low, parts, preferred_element_type=F32
        )
        attention = jnp.concatenate(
            [att_rows[pl.ds(h, batch, stride=heads), :] for h in range(heads)], axis=1
        ).astype(BF16)
        for core in range(n_c):
            proj_mine[core] = jnp.dot(
                attention, w_ref[core], preferred_element_type=F32
            ).astype(BF16)
        proj_all[x] = proj_mine[top]

        pl.semaphore_wait(side_sem.at[1], 2)
        for dx in sorted(range(n_x), key=lambda d: -min(d, n_x - d)):
            for core in range(n_c):
                if dx == 0 and core == top:
                    continue
                pltpu.make_async_remote_copy(
                    src_ref=proj_mine.at[core],
                    dst_ref=proj_all.at[x],
                    send_sem=c_send.at[core],
                    recv_sem=c_recv,
                    device_id={"head": lax.rem(x + dx, n_x), "sub": core},
                    device_id_type=MESH,
                ).start()
        wait_all(all_lse, (n_z - 1) * per, b_send.at[1])
        wait_all(all_out, n_z - 1, b_send.at[0])
        wait_all(proj_all, n_x, c_send.at[0])
        wait_all(proj_all, n_x - 1, c_send.at[top])
        wait_all(proj_all, n_x - 1, c_recv)

    pl.when(c != top)(other_core)
    pl.when(c == top)(top_core)
    summed = proj_all[0].astype(F32)
    for i in range(1, n_x):
        summed = summed + proj_all[i].astype(F32)
    out_ref[...] = summed.astype(out_ref.dtype)


def on_device(sizes, queries, key_cache, value_cache, seq_lengths, slot_owner, slot_page, out_weight):
    n_z, n_x, n_c = sizes
    batch, heads = queries.shape[0], queries.shape[1] // DH
    slots = key_cache.shape[0]
    rows = batch * heads
    width = out_weight.shape[1]
    sources = n_z // COPIES * n_c
    per = batch // (n_z // COPIES)
    assert key_cache.shape[2] == DH and rows == DH and n_c == 2
    hbm = pl.BlockSpec(memory_space=pltpu.HBM)
    dma = pltpu.SemaphoreType.DMA
    return pl.pallas_call(
        functools.partial(kernel, sizes),
        out_shape=pltpu.VMEM((batch, width), BF16),
        in_specs=[hbm] * 8,
        out_specs=pl.BlockSpec(memory_space=pltpu.VMEM),
        scratch_shapes=[
            pltpu.SMEM((batch,), jnp.int32),
            pltpu.SMEM((slots,), jnp.int32),
            pltpu.SMEM((slots,), jnp.int32),
            pltpu.VMEM((1, slots), jnp.int32),
            pltpu.VMEM(queries.shape, BF16),
            pltpu.VMEM(key_cache.shape, BF16),
            pltpu.VMEM(value_cache.shape, BF16),
            pltpu.VMEM((n_c, *out_weight.shape), BF16),
            pltpu.VMEM((rows, DH), F32),
            pltpu.VMEM((batch, heads, DH), F32),
            pltpu.VMEM((slots * heads, PAGE), F32),
            pltpu.VMEM((slots * heads, PAGE), F32),
            pltpu.VMEM((rows, slots * heads), BF16),
            pltpu.VMEM((batch, heads, rows), F32),
            pltpu.VMEM((rows, rows), F32),
            pltpu.VMEM((batch // per, per, heads, DH), BF16),
            pltpu.VMEM((batch, rows), F32),
            pltpu.VMEM((sources, per, heads, DH), BF16),
            pltpu.VMEM((sources * per, rows), F32),
            pltpu.VMEM((per, heads, DH), BF16),
            pltpu.VMEM((per, rows), F32),
            pltpu.VMEM((n_z, per, heads, DH), BF16),
            pltpu.VMEM((n_z * per, rows), F32),
            pltpu.VMEM((rows, DH), F32),
            pltpu.VMEM((n_c, batch, width), BF16),
            pltpu.VMEM((n_x, batch, width), BF16),
            dma((5,)),
            dma,
            dma,
            dma,
            dma((2,)),
            dma((2,)),
            dma((2,)),
            dma((2,)),
            dma((2,)),
            dma((n_c,)),
            dma,
            pltpu.SemaphoreType.REGULAR,
            pltpu.SemaphoreType.REGULAR((2,)),
        ],
        compiler_params=pltpu.CompilerParams(collective_id=0, has_side_effects=True),
        name="decode",
    )(
        seq_lengths,
        slot_owner,
        slot_page,
        slot_owner.reshape(1, slots),
        queries,
        key_cache,
        value_cache,
        out_weight,
    )


def solution(mesh):
    sizes = (mesh.shape["seq"], mesh.shape["head"], mesh.shape["sub"])
    in_specs = (
        P("rep", "head"),
        P(("rep", "seq", "sub"), None, "head"),
        P(("rep", "seq", "sub"), None, "head"),
        P("rep"),
        P(("rep", "seq", "sub")),
        P(("rep", "seq", "sub")),
        P("head", ("seq", "sub")),
    )
    out_specs = P("rep", ("seq", "sub"))
    return jax.shard_map(
        functools.partial(on_device, sizes),
        mesh=mesh,
        in_specs=in_specs,
        out_specs=out_specs,
        check_vma=False,
    )
```

```python
import functools

import jax
import jax.numpy as jnp
from jax import lax
from jax.experimental import pallas as pl
from jax.experimental.pallas import tpu as pltpu
from jax.sharding import PartitionSpec as P

DH = 128
PAGE = 128
NEG = -1e30
COPIES = 4
F32 = jnp.float32
BF16 = jnp.bfloat16
MESH = pl.DeviceIdType.MESH


def kernel(
    sizes,
    lengths_hbm,
    owners_hbm,
    numbers_hbm,
    owner_row_hbm,
    q_hbm,
    k_hbm,
    v_hbm,
    w_hbm,
    out_ref,
    lengths,
    owners,
    numbers,
    owner_row,
    q_ref,
    k_ref,
    v_ref,
    w_ref,
    q_rows,
    q_seq,
    peaks,
    masses,
    hits,
    seq_lse,
    lse_diag,
    part_out,
    part_lse,
    got_out,
    got_lse,
    own_out,
    own_lse,
    all_out,
    all_lse,
    att_rows,
    proj_mine,
    proj_all,
    small_sem,
    k_sem,
    v_sem,
    w_sem,
    w_pass,
    a_send,
    a_recv,
    b_send,
    b_recv,
    c_send,
    c_recv,
    far_sem,
    side_sem,
):
    n_z, n_x, n_c = sizes
    batch, heads, slots = lengths.shape[0], q_ref.shape[1] // DH, owners.shape[0]
    half = n_z // 2
    near = half // 2
    seg = n_z // COPIES
    per = batch // seg
    top = n_c - 1
    sources = seg * n_c
    z, x, c = lax.axis_index("seq"), lax.axis_index("head"), lax.axis_index("sub")
    rows = batch * heads

    def ring(offset):
        return lax.rem(z + offset + n_z, n_z)

    small = [
        pltpu.make_async_copy(src, dst, small_sem.at[i])
        for i, (src, dst) in enumerate(
            (
                (owners_hbm, owners),
                (lengths_hbm, lengths),
                (numbers_hbm, numbers),
                (owner_row_hbm, owner_row),
                (q_hbm, q_ref),
            )
        )
    ]
    k_load = pltpu.make_async_copy(k_hbm, k_ref, k_sem)
    v_load = pltpu.make_async_copy(v_hbm, v_ref, v_sem)
    w_load = pltpu.make_async_copy(w_hbm, w_ref.at[top], w_sem)
    for copy in small + [k_load, v_load]:
        copy.start()

    def wait_all(ref, count, sem):
        span = ref.at[pl.ds(0, count)]
        pltpu.make_async_copy(span, span, sem).wait()

    barrier = pltpu.get_barrier_semaphore()

    def greet(**where):
        pl.semaphore_signal(barrier, inc=1, device_id=where, device_id_type=MESH)

    @pl.when(c == top)
    def _():
        for dz in sorted(range(-near, near + 1), key=lambda d: -abs(d)):
            for core in range(n_c):
                if dz or core != top:
                    greet(seq=ring(dz), sub=core)
        for dx in (1, n_x - 1):
            greet(head=lax.rem(x + dx, n_x), sub=top)

    @pl.when(c != top)
    def _():
        for dx in (0, 1, n_x - 1):
            greet(head=lax.rem(x + dx, n_x), sub=top)

    greeted_top = 2 * near + (n_c - 1) + 2 * n_c
    greeted_other = 2 * near + 1

    for copy in small:
        copy.wait()

    lane = lax.broadcasted_iota(jnp.int32, (heads, rows), 1)
    sub = lax.broadcasted_iota(jnp.int32, (heads, rows), 0)
    diag = lane - sub

    for h in range(heads):
        q_rows[pl.ds(h, batch, stride=heads), :] = q_ref[:, h * DH : (h + 1) * DH].astype(F32)
    q_seq[...] = q_rows[...].reshape(batch, heads, DH)

    hit = (lax.broadcasted_iota(jnp.int32, (batch, slots), 0) == owner_row[...]).astype(BF16)
    spread_rows = lax.broadcasted_iota(jnp.int32, (slots, slots * heads), 0)
    spread_cols = lax.broadcasted_iota(jnp.int32, (slots, slots * heads), 1)
    spread = (spread_cols // heads == spread_rows).astype(BF16)
    wide = jnp.dot(hit, spread, preferred_element_type=F32)
    wide = jnp.broadcast_to(wide[:, None, :], (batch, heads, slots * heads))
    w_sub = lax.broadcasted_iota(jnp.int32, (batch, heads, slots * heads), 1)
    w_lane = lax.broadcasted_iota(jnp.int32, (batch, heads, slots * heads), 2)
    hits[...] = jnp.where(w_lane % heads == w_sub, wide, 0.0).reshape(rows, slots * heads).astype(BF16)

    scale = 1.0 / (float(DH) ** 0.5)
    pair_sub = lax.broadcasted_iota(jnp.int32, (2 * heads, PAGE), 0)
    pair_lane = lax.broadcasted_iota(jnp.int32, (2 * heads, PAGE), 1)
    first = pair_sub < heads

    probs = []
    peak_diag = jnp.full((heads, rows), NEG, F32)
    k_load.wait()
    for pair in range(slots // 2):
        a, b = 2 * pair, 2 * pair + 1
        own_a, own_b = owners[a], owners[b]
        q_pair = jnp.concatenate(
            [
                q_seq[own_a],
                q_seq[own_b],
            ],
            axis=0,
        ).astype(BF16)
        keys = k_ref[a : b + 1].reshape(2 * PAGE, DH)
        both = lax.dot_general(
            q_pair, keys, (((1,), (1,)), ((), ())), preferred_element_type=F32
        )
        scores = jnp.concatenate([both[:heads, :PAGE], both[heads:, PAGE:]], axis=0) * scale
        live_a = jnp.clip(lengths[own_a] - numbers[a] * PAGE, 0, PAGE)
        live_b = jnp.clip(lengths[own_b] - numbers[b] * PAGE, 0, PAGE)
        scores = jnp.where(pair_lane < jnp.where(first, live_a, live_b), scores, NEG)
        peak = jnp.max(scores, axis=1, keepdims=True)
        prob = jnp.exp(scores - peak).astype(BF16)
        mass = jnp.sum(prob.astype(F32), axis=1, keepdims=True)
        peak = jnp.broadcast_to(peak, (2 * heads, PAGE))
        mass = jnp.broadcast_to(mass, (2 * heads, PAGE))
        peaks[pl.ds(a * heads, 2 * heads), :] = peak
        masses[pl.ds(a * heads, 2 * heads), :] = mass
        probs.append(prob)
        peak_diag = jnp.maximum(peak_diag, jnp.where(diag == own_a * heads, peak[:heads], NEG))
        peak_diag = jnp.maximum(peak_diag, jnp.where(diag == own_b * heads, peak[heads:], NEG))

    v_load.wait()

    def by_sequence(row_values):
        for b in range(batch):
            mine = jnp.max(
                jnp.where(lane // heads == b, row_values, 2 * NEG), axis=1, keepdims=True
            )
            seq_lse[b] = jnp.broadcast_to(mine, (heads, rows))

    by_sequence(peak_diag)
    total = jnp.zeros((heads, rows), F32)
    for s in range(slots):
        span = pl.ds(s * heads, heads)
        factor = jnp.exp(peaks[span, :] - seq_lse[owners[s]])
        total = total + jnp.where(diag == owners[s] * heads, factor * masses[span, :], 0.0)
    lse = jnp.where(total > 0.0, peak_diag + jnp.log(jnp.where(total > 0.0, total, 1.0)), NEG)
    by_sequence(lse)

    for b in range(batch):
        lse_diag[pl.ds(b * heads, heads), :] = jnp.where(lane % heads == sub, seq_lse[b], 0.0)
    tiled = lse_diag[pl.ds(0, batch, stride=heads), :]
    for h in range(1, heads):
        tiled = tiled + lse_diag[pl.ds(h, batch, stride=heads), :]
    part_lse[...] = tiled

    high, low = [], []
    for pair in range(slots // 2):
        a, b = 2 * pair, 2 * pair + 1
        prob = probs[pair]
        block = jnp.concatenate(
            [
                jnp.where(first, prob, jnp.zeros_like(prob)),
                jnp.where(first, jnp.zeros_like(prob), prob),
            ],
            axis=1,
        )
        values = v_ref[a : b + 1].reshape(2 * PAGE, DH)
        page_out = jnp.dot(block, values, preferred_element_type=F32)
        span = pl.ds(a * heads, 2 * heads)
        level = jnp.concatenate([seq_lse[owners[a]], seq_lse[owners[b]]], axis=0)
        factor = jnp.exp(peaks[span, :] - level)
        page_out = page_out * factor
        high.append(page_out.astype(BF16))
        low.append((page_out - high[-1].astype(F32)).astype(BF16))
    hit = hits[...]
    mine = jnp.dot(hit, jnp.concatenate(high, axis=0), preferred_element_type=F32)
    mine = mine + jnp.dot(hit, jnp.concatenate(low, axis=0), preferred_element_type=F32)
    part_out[...] = mine.astype(BF16).reshape(seg, per, heads, DH)

    def send_parts(core):
        sent = 0
        for dz in sorted(range(-(seg // 2), seg // 2), key=lambda d: -abs(d)):
            target = lax.rem(ring(dz), seg)
            slot = (seg // 2 - 1 - dz) * n_c + core
            src_rows, dst_rows = pl.ds(target * per, per), pl.ds(slot * per, per)
            if dz == 0 and core == top:
                got_out[slot] = part_out[target]
                got_lse[dst_rows, :] = part_lse[src_rows, :]
                continue
            for k, (src, dst) in enumerate(
                (
                    (part_out.at[target], got_out.at[slot]),
                    (part_lse.at[src_rows, :], got_lse.at[dst_rows, :]),
                )
            ):
                pltpu.make_async_remote_copy(
                    src_ref=src,
                    dst_ref=dst,
                    send_sem=a_send.at[k],
                    recv_sem=a_recv.at[k],
                    device_id={"seq": ring(dz), "sub": top},
                    device_id_type=MESH,
                ).start()
            sent += 1
        return sent

    def other_core():
        pl.semaphore_wait(barrier, greeted_other)
        sent = send_parts(0)
        weights = pltpu.make_async_remote_copy(
            src_ref=w_hbm,
            dst_ref=w_ref.at[0],
            send_sem=w_pass.at[0],
            recv_sem=w_pass.at[1],
            device_id={"sub": top},
            device_id_type=MESH,
        )
        weights.start()
        wait_all(part_lse, sent * per, a_send.at[1])
        wait_all(part_out, sent, a_send.at[0])
        weights.wait_send()
        wait_all(proj_all, n_x, c_recv)

    def top_core():
        pl.semaphore_wait(barrier, greeted_top)
        for dz in (-near, near):
            pl.semaphore_signal(far_sem, inc=1, device_id={"seq": ring(dz)}, device_id_type=MESH)
        sent = send_parts(top)
        w_load.start()
        for dx in (1, n_x - 1):
            pl.semaphore_signal(
                side_sem.at[0], inc=1, device_id={"head": lax.rem(x + dx, n_x)}, device_id_type=MESH
            )
        wait_all(got_lse, (sources - 1) * per, a_recv.at[1])
        wait_all(got_out, sources - 1, a_recv.at[0])

        wide_rows = rows * n_c
        s_sub = lax.broadcasted_iota(jnp.int32, (sources, wide_rows), 0)
        s_lane = lax.broadcasted_iota(jnp.int32, (sources, wide_rows), 1)
        m_lane = lax.broadcasted_iota(jnp.int32, (heads, wide_rows), 1)
        m_sub = lax.broadcasted_iota(jnp.int32, (heads, wide_rows), 0)
        mixes = []
        for i in range(per):
            levels = got_lse[pl.ds(i, sources, stride=per), :]
            peak = jnp.max(levels, axis=0, keepdims=True)
            weight = jnp.exp(levels - peak)
            norm = jnp.sum(weight, axis=0, keepdims=True)
            weight = jnp.concatenate([weight / norm] * n_c, axis=1)
            flat = jnp.sum(
                jnp.where(s_lane // heads == s_sub * per + i, weight, 0.0), axis=0, keepdims=True
            )
            mixes.append(jnp.where(m_lane % heads == m_sub, jnp.broadcast_to(flat, (heads, wide_rows)), 0.0))
            own_lse[pl.ds(i, 1), :] = peak + jnp.log(norm)
        mix = jnp.concatenate(mixes, axis=0)
        high = mix.astype(BF16)
        low = (mix - high.astype(F32)).astype(BF16)
        parts = got_out[...].reshape(wide_rows, DH)
        own = jnp.dot(high, parts, preferred_element_type=F32) + jnp.dot(
            low, parts, preferred_element_type=F32
        )
        own_out[...] = own.astype(BF16).reshape(per, heads, DH)

        pl.semaphore_wait(far_sem, 2)
        b_rows = pl.ds(z * per, per)
        all_out[z] = own_out[...]
        all_lse[b_rows, :] = own_lse[...]
        for dz in sorted(range(-half + 1, half + 1), key=lambda d: -abs(d)):
            if dz == 0:
                continue
            for k, (src, dst) in enumerate(
                ((own_out, all_out.at[z]), (own_lse, all_lse.at[b_rows, :]))
            ):
                pltpu.make_async_remote_copy(
                    src_ref=src,
                    dst_ref=dst,
                    send_sem=b_send.at[k],
                    recv_sem=b_recv.at[k],
                    device_id={"seq": ring(dz)},
                    device_id_type=MESH,
                ).start()
        pl.semaphore_wait(side_sem.at[0], 2)
        for dx in (2, n_x - 2):
            pl.semaphore_signal(
                side_sem.at[1], inc=1, device_id={"head": lax.rem(x + dx, n_x)}, device_id_type=MESH
            )
        w_load.wait()
        pltpu.make_async_copy(w_ref.at[0], w_ref.at[0], w_pass.at[1]).wait()
        wait_all(part_lse, sent * per, a_send.at[1])
        wait_all(part_out, sent, a_send.at[0])
        wait_all(all_lse, (n_z - 1) * per, b_recv.at[1])
        wait_all(all_out, n_z - 1, b_recv.at[0])

        levels = [all_lse[i * batch : (i + 1) * batch, :] for i in range(COPIES)]
        peak = functools.reduce(jnp.maximum, levels)
        weights = [jnp.exp(level - peak) for level in levels]
        inv = 1.0 / sum(weights)
        spot = lax.broadcasted_iota(jnp.int32, (batch, heads, rows), 0) * heads
        spot = spot + lax.broadcasted_iota(jnp.int32, (batch, heads, rows), 1)
        here = lax.broadcasted_iota(jnp.int32, (batch, heads, rows), 2) == spot
        blocks = []
        for weight in weights:
            expanded = jnp.broadcast_to((weight * inv)[:, None, :], (batch, heads, rows))
            blocks.append(jnp.where(here, expanded, 0.0).reshape(rows, rows))
        mix = jnp.concatenate(blocks, axis=1)
        high = mix.astype(BF16)
        low = (mix - high.astype(F32)).astype(BF16)
        parts = all_out[...].reshape(COPIES * rows, DH)
        att_rows[...] = jnp.dot(high, parts, preferred_element_type=F32) + jnp.dot(
            low, parts, preferred_element_type=F32
        )
        attention = jnp.concatenate(
            [att_rows[pl.ds(h, batch, stride=heads), :] for h in range(heads)], axis=1
        ).astype(BF16)
        for core in range(n_c):
            proj_mine[core] = jnp.dot(
                attention, w_ref[core], preferred_element_type=F32
            ).astype(BF16)
        proj_all[x] = proj_mine[top]

        pl.semaphore_wait(side_sem.at[1], 2)
        for dx in sorted(range(n_x), key=lambda d: -min(d, n_x - d)):
            for core in range(n_c):
                if dx == 0 and core == top:
                    continue
                pltpu.make_async_remote_copy(
                    src_ref=proj_mine.at[core],
                    dst_ref=proj_all.at[x],
                    send_sem=c_send.at[core],
                    recv_sem=c_recv,
                    device_id={"head": lax.rem(x + dx, n_x), "sub": core},
                    device_id_type=MESH,
                ).start()
        wait_all(all_lse, (n_z - 1) * per, b_send.at[1])
        wait_all(all_out, n_z - 1, b_send.at[0])
        wait_all(proj_all, n_x, c_send.at[0])
        wait_all(proj_all, n_x - 1, c_send.at[top])
        wait_all(proj_all, n_x - 1, c_recv)

    pl.when(c != top)(other_core)
    pl.when(c == top)(top_core)
    summed = proj_all[0].astype(F32)
    for i in range(1, n_x):
        summed = summed + proj_all[i].astype(F32)
    out_ref[...] = summed.astype(out_ref.dtype)


def on_device(sizes, queries, key_cache, value_cache, seq_lengths, slot_owner, slot_page, out_weight):
    n_z, n_x, n_c = sizes
    batch, heads = queries.shape[0], queries.shape[1] // DH
    slots = key_cache.shape[0]
    rows = batch * heads
    width = out_weight.shape[1]
    sources = n_z // COPIES * n_c
    per = batch // (n_z // COPIES)
    assert key_cache.shape[2] == DH and rows == DH and n_c == 2
    hbm = pl.BlockSpec(memory_space=pltpu.HBM)
    dma = pltpu.SemaphoreType.DMA
    return pl.pallas_call(
        functools.partial(kernel, sizes),
        out_shape=pltpu.VMEM((batch, width), BF16),
        in_specs=[hbm] * 8,
        out_specs=pl.BlockSpec(memory_space=pltpu.VMEM),
        scratch_shapes=[
            pltpu.SMEM((batch,), jnp.int32),
            pltpu.SMEM((slots,), jnp.int32),
            pltpu.SMEM((slots,), jnp.int32),
            pltpu.VMEM((1, slots), jnp.int32),
            pltpu.VMEM(queries.shape, BF16),
            pltpu.VMEM(key_cache.shape, BF16),
            pltpu.VMEM(value_cache.shape, BF16),
            pltpu.VMEM((n_c, *out_weight.shape), BF16),
            pltpu.VMEM((rows, DH), F32),
            pltpu.VMEM((batch, heads, DH), F32),
            pltpu.VMEM((slots * heads, PAGE), F32),
            pltpu.VMEM((slots * heads, PAGE), F32),
            pltpu.VMEM((rows, slots * heads), BF16),
            pltpu.VMEM((batch, heads, rows), F32),
            pltpu.VMEM((rows, rows), F32),
            pltpu.VMEM((batch // per, per, heads, DH), BF16),
            pltpu.VMEM((batch, rows), F32),
            pltpu.VMEM((sources, per, heads, DH), BF16),
            pltpu.VMEM((sources * per, rows), F32),
            pltpu.VMEM((per, heads, DH), BF16),
            pltpu.VMEM((per, rows), F32),
            pltpu.VMEM((n_z, per, heads, DH), BF16),
            pltpu.VMEM((n_z * per, rows), F32),
            pltpu.VMEM((rows, DH), F32),
            pltpu.VMEM((n_c, batch, width), BF16),
            pltpu.VMEM((n_x, batch, width), BF16),
            dma((5,)),
            dma,
            dma,
            dma,
            dma((2,)),
            dma((2,)),
            dma((2,)),
            dma((2,)),
            dma((2,)),
            dma((n_c,)),
            dma,
            pltpu.SemaphoreType.REGULAR,
            pltpu.SemaphoreType.REGULAR((2,)),
        ],
        compiler_params=pltpu.CompilerParams(collective_id=0, has_side_effects=True),
        name="decode",
    )(
        seq_lengths,
        slot_owner,
        slot_page,
        slot_owner.reshape(1, slots),
        queries,
        key_cache,
        value_cache,
        out_weight,
    )


def solution(mesh):
    sizes = (mesh.shape["seq"], mesh.shape["head"], mesh.shape["sub"])
    in_specs = (
        P("rep", "head"),
        P(("rep", "seq", "sub"), None, "head"),
        P(("rep", "seq", "sub"), None, "head"),
        P("rep"),
        P(("rep", "seq", "sub")),
        P(("rep", "seq", "sub")),
        P("head", ("seq", "sub")),
    )
    out_specs = P("rep", ("seq", "sub"))
    return jax.shard_map(
        functools.partial(on_device, sizes),
        mesh=mesh,
        in_specs=in_specs,
        out_specs=out_specs,
        check_vma=False,
    )
```

```python
import functools

import jax
import jax.numpy as jnp
from jax import lax
from jax.experimental import pallas as pl
from jax.experimental.pallas import tpu as pltpu
from jax.sharding import PartitionSpec as P

DH = 128
PAGE = 128
NEG = -1e30
COPIES = 4
F32 = jnp.float32
BF16 = jnp.bfloat16
MESH = pl.DeviceIdType.MESH


def kernel(
    sizes,
    lengths_hbm,
    owners_hbm,
    numbers_hbm,
    owner_row_hbm,
    q_hbm,
    k_hbm,
    v_hbm,
    w_hbm,
    out_ref,
    lengths,
    owners,
    numbers,
    owner_row,
    q_ref,
    k_ref,
    v_ref,
    w_ref,
    q_rows,
    q_seq,
    peaks,
    masses,
    hits,
    seq_peak,
    seq_lse,
    lse_diag,
    part_out,
    part_lse,
    got_out,
    got_lse,
    own_out,
    own_lse,
    all_out,
    all_lse,
    att_rows,
    proj_mine,
    proj_all,
    small_sem,
    k_sem,
    v_sem,
    w_sem,
    w_pass,
    a_send,
    a_recv,
    b_send,
    b_recv,
    c_send,
    c_recv,
    far_sem,
    side_sem,
):
    n_z, n_x, n_c = sizes
    batch, heads, slots = lengths.shape[0], q_ref.shape[1] // DH, owners.shape[0]
    half = n_z // 2
    near = half // 2
    seg = n_z // COPIES
    per = batch // seg
    top = n_c - 1
    sources = seg * n_c
    z, x, c = lax.axis_index("seq"), lax.axis_index("head"), lax.axis_index("sub")
    rows = batch * heads

    def ring(offset):
        return lax.rem(z + offset + n_z, n_z)

    small = [
        pltpu.make_async_copy(src, dst, small_sem.at[i])
        for i, (src, dst) in enumerate(
            (
                (owners_hbm, owners),
                (lengths_hbm, lengths),
                (numbers_hbm, numbers),
                (owner_row_hbm, owner_row),
                (q_hbm, q_ref),
            )
        )
    ]
    k_load = pltpu.make_async_copy(k_hbm, k_ref, k_sem)
    v_load = pltpu.make_async_copy(v_hbm, v_ref, v_sem)
    w_load = pltpu.make_async_copy(w_hbm, w_ref.at[top], w_sem)
    for copy in small + [k_load, v_load]:
        copy.start()

    def wait_all(ref, count, sem):
        span = ref.at[pl.ds(0, count)]
        pltpu.make_async_copy(span, span, sem).wait()

    barrier = pltpu.get_barrier_semaphore()

    def greet(**where):
        pl.semaphore_signal(barrier, inc=1, device_id=where, device_id_type=MESH)

    @pl.when(c == top)
    def _():
        for dz in sorted(range(-near, near + 1), key=lambda d: -abs(d)):
            for core in range(n_c):
                if dz or core != top:
                    greet(seq=ring(dz), sub=core)
        for dx in (1, n_x - 1):
            greet(head=lax.rem(x + dx, n_x), sub=top)

    @pl.when(c != top)
    def _():
        for dx in (0, 1, n_x - 1):
            greet(head=lax.rem(x + dx, n_x), sub=top)

    greeted_top = 2 * near + (n_c - 1) + 2 * n_c
    greeted_other = 2 * near + 1

    for copy in small:
        copy.wait()

    lane = lax.broadcasted_iota(jnp.int32, (heads, rows), 1)
    sub = lax.broadcasted_iota(jnp.int32, (heads, rows), 0)
    diag = lane - sub

    for h in range(heads):
        q_rows[pl.ds(h, batch, stride=heads), :] = q_ref[:, h * DH : (h + 1) * DH].astype(F32)
    q_seq[...] = q_rows[...].reshape(batch, heads, DH)

    hit = (lax.broadcasted_iota(jnp.int32, (batch, slots), 0) == owner_row[...]).astype(BF16)
    spread_rows = lax.broadcasted_iota(jnp.int32, (slots, slots * heads), 0)
    spread_cols = lax.broadcasted_iota(jnp.int32, (slots, slots * heads), 1)
    spread = (spread_cols // heads == spread_rows).astype(BF16)
    wide = jnp.dot(hit, spread, preferred_element_type=F32)
    wide = jnp.broadcast_to(wide[:, None, :], (batch, heads, slots * heads))
    w_sub = lax.broadcasted_iota(jnp.int32, (batch, heads, slots * heads), 1)
    w_lane = lax.broadcasted_iota(jnp.int32, (batch, heads, slots * heads), 2)
    hits[...] = jnp.where(w_lane % heads == w_sub, wide, 0.0).reshape(rows, slots * heads).astype(BF16)

    scale = 1.0 / (float(DH) ** 0.5)
    pair_sub = lax.broadcasted_iota(jnp.int32, (2 * heads, PAGE), 0)
    pair_lane = lax.broadcasted_iota(jnp.int32, (2 * heads, PAGE), 1)
    first = pair_sub < heads

    probs = []
    peak_diag = jnp.full((heads, rows), NEG, F32)
    k_load.wait()
    for pair in range(slots // 2):
        a, b = 2 * pair, 2 * pair + 1
        own_a, own_b = owners[a], owners[b]
        q_pair = jnp.concatenate(
            [
                q_seq[own_a],
                q_seq[own_b],
            ],
            axis=0,
        ).astype(BF16)
        keys = k_ref[a : b + 1].reshape(2 * PAGE, DH)
        both = lax.dot_general(
            q_pair, keys, (((1,), (1,)), ((), ())), preferred_element_type=F32
        )
        scores = jnp.concatenate([both[:heads, :PAGE], both[heads:, PAGE:]], axis=0) * scale
        live_a = jnp.clip(lengths[own_a] - numbers[a] * PAGE, 0, PAGE)
        live_b = jnp.clip(lengths[own_b] - numbers[b] * PAGE, 0, PAGE)
        scores = jnp.where(pair_lane < jnp.where(first, live_a, live_b), scores, NEG)
        peak = jnp.max(scores, axis=1, keepdims=True)
        prob = jnp.exp(scores - peak).astype(BF16)
        mass = jnp.sum(prob.astype(F32), axis=1, keepdims=True)
        peak = jnp.broadcast_to(peak, (2 * heads, PAGE))
        mass = jnp.broadcast_to(mass, (2 * heads, PAGE))
        peaks[pl.ds(a * heads, 2 * heads), :] = peak
        masses[pl.ds(a * heads, 2 * heads), :] = mass
        probs.append(prob)
        peak_diag = jnp.maximum(peak_diag, jnp.where(diag == own_a * heads, peak[:heads], NEG))
        peak_diag = jnp.maximum(peak_diag, jnp.where(diag == own_b * heads, peak[heads:], NEG))


    @pl.when(c == top)
    def _():
        pl.semaphore_wait(barrier, greeted_top)
        for dz in (-near, near):
            pl.semaphore_signal(far_sem, inc=1, device_id={"seq": ring(dz)}, device_id_type=MESH)
        for dx in (1, n_x - 1):
            pl.semaphore_signal(
                side_sem.at[0], inc=1, device_id={"head": lax.rem(x + dx, n_x)}, device_id_type=MESH
            )

    @pl.when(c != top)
    def _():
        pl.semaphore_wait(barrier, greeted_other)

    v_load.wait()

    def by_sequence(row_values, ref):
        for b in range(batch):
            mine = jnp.max(
                jnp.where(lane // heads == b, row_values, 2 * NEG), axis=1, keepdims=True
            )
            ref[b] = jnp.broadcast_to(mine, (heads, rows))

    by_sequence(peak_diag, seq_peak)
    total = jnp.zeros((heads, rows), F32)
    factors = []
    for s in range(slots):
        span = pl.ds(s * heads, heads)
        factors.append(jnp.exp(peaks[span, :] - seq_peak[owners[s]]))
        total = total + jnp.where(diag == owners[s] * heads, factors[s] * masses[span, :], 0.0)
    lse = jnp.where(
        total > 0.0, peak_diag + jnp.log(jnp.where(total > 0.0, total, 1.0)), NEG
    )
    by_sequence(lse, seq_lse)

    for b in range(batch):
        lse_diag[pl.ds(b * heads, heads), :] = jnp.where(lane % heads == sub, seq_lse[b], 0.0)
    tiled = lse_diag[pl.ds(0, batch, stride=heads), :]
    for h in range(1, heads):
        tiled = tiled + lse_diag[pl.ds(h, batch, stride=heads), :]
    part_lse[...] = tiled

    high, low = [], []
    for pair in range(slots // 2):
        a, b = 2 * pair, 2 * pair + 1
        prob = probs[pair]
        block = jnp.concatenate(
            [
                jnp.where(first, prob, jnp.zeros_like(prob)),
                jnp.where(first, jnp.zeros_like(prob), prob),
            ],
            axis=1,
        )
        values = v_ref[a : b + 1].reshape(2 * PAGE, DH)
        page_out = jnp.dot(block, values, preferred_element_type=F32)
        page_out = page_out * jnp.concatenate([factors[a], factors[b]], axis=0)
        high.append(page_out.astype(BF16))
        low.append((page_out - high[-1].astype(F32)).astype(BF16))
    hit = hits[...]
    mine = jnp.dot(hit, jnp.concatenate(high, axis=0), preferred_element_type=F32)
    mine = mine + jnp.dot(hit, jnp.concatenate(low, axis=0), preferred_element_type=F32)
    mine = mine * jnp.exp(seq_peak[...] - seq_lse[...]).reshape(rows, rows)
    part_out[...] = mine.astype(BF16).reshape(seg, per, heads, DH)

    def send_parts(core):
        sent = 0
        for dz in sorted(range(-(seg // 2), seg // 2), key=lambda d: -abs(d)):
            target = lax.rem(ring(dz), seg)
            slot = (seg // 2 - 1 - dz) * n_c + core
            src_rows, dst_rows = pl.ds(target * per, per), pl.ds(slot * per, per)
            if dz == 0 and core == top:
                got_out[slot] = part_out[target]
                got_lse[dst_rows, :] = part_lse[src_rows, :]
                continue
            for k, (src, dst) in enumerate(
                (
                    (part_out.at[target], got_out.at[slot]),
                    (part_lse.at[src_rows, :], got_lse.at[dst_rows, :]),
                )
            ):
                pltpu.make_async_remote_copy(
                    src_ref=src,
                    dst_ref=dst,
                    send_sem=a_send.at[k],
                    recv_sem=a_recv.at[k],
                    device_id={"seq": ring(dz), "sub": top},
                    device_id_type=MESH,
                ).start()
            sent += 1
        return sent

    def other_core():
        sent = send_parts(0)
        weights = pltpu.make_async_remote_copy(
            src_ref=w_hbm,
            dst_ref=w_ref.at[0],
            send_sem=w_pass.at[0],
            recv_sem=w_pass.at[1],
            device_id={"sub": top},
            device_id_type=MESH,
        )
        weights.start()
        wait_all(part_lse, sent * per, a_send.at[1])
        wait_all(part_out, sent, a_send.at[0])
        weights.wait_send()
        wait_all(proj_all, n_x, c_recv)

    def top_core():
        sent = send_parts(top)
        w_load.start()
        wait_all(got_lse, (sources - 1) * per, a_recv.at[1])
        wait_all(got_out, sources - 1, a_recv.at[0])

        wide_rows = rows * n_c
        s_sub = lax.broadcasted_iota(jnp.int32, (sources, wide_rows), 0)
        s_lane = lax.broadcasted_iota(jnp.int32, (sources, wide_rows), 1)
        m_lane = lax.broadcasted_iota(jnp.int32, (heads, wide_rows), 1)
        m_sub = lax.broadcasted_iota(jnp.int32, (heads, wide_rows), 0)
        mixes = []
        for i in range(per):
            levels = got_lse[pl.ds(i, sources, stride=per), :]
            peak = jnp.max(levels, axis=0, keepdims=True)
            weight = jnp.exp(levels - peak)
            norm = jnp.sum(weight, axis=0, keepdims=True)
            weight = jnp.concatenate([weight / norm] * n_c, axis=1)
            flat = jnp.sum(
                jnp.where(s_lane // heads == s_sub * per + i, weight, 0.0), axis=0, keepdims=True
            )
            mixes.append(jnp.where(m_lane % heads == m_sub, jnp.broadcast_to(flat, (heads, wide_rows)), 0.0))
            own_lse[pl.ds(i, 1), :] = peak + jnp.log(norm)
        mix = jnp.concatenate(mixes, axis=0)
        high = mix.astype(BF16)
        low = (mix - high.astype(F32)).astype(BF16)
        parts = got_out[...].reshape(wide_rows, DH)
        own = jnp.dot(high, parts, preferred_element_type=F32) + jnp.dot(
            low, parts, preferred_element_type=F32
        )
        own_out[...] = own.astype(BF16).reshape(per, heads, DH)

        pl.semaphore_wait(far_sem, 2)
        b_rows = pl.ds(z * per, per)
        all_out[z] = own_out[...]
        all_lse[b_rows, :] = own_lse[...]
        for dz in sorted(range(-half + 1, half + 1), key=lambda d: -abs(d)):
            if dz == 0:
                continue
            for k, (src, dst) in enumerate(
                ((own_out, all_out.at[z]), (own_lse, all_lse.at[b_rows, :]))
            ):
                pltpu.make_async_remote_copy(
                    src_ref=src,
                    dst_ref=dst,
                    send_sem=b_send.at[k],
                    recv_sem=b_recv.at[k],
                    device_id={"seq": ring(dz)},
                    device_id_type=MESH,
                ).start()
        pl.semaphore_wait(side_sem.at[0], 2)
        for dx in (2, n_x - 2):
            pl.semaphore_signal(
                side_sem.at[1], inc=1, device_id={"head": lax.rem(x + dx, n_x)}, device_id_type=MESH
            )
        w_load.wait()
        pltpu.make_async_copy(w_ref.at[0], w_ref.at[0], w_pass.at[1]).wait()
        wait_all(part_lse, sent * per, a_send.at[1])
        wait_all(part_out, sent, a_send.at[0])
        wait_all(all_lse, (n_z - 1) * per, b_recv.at[1])
        wait_all(all_out, n_z - 1, b_recv.at[0])

        levels = [all_lse[i * batch : (i + 1) * batch, :] for i in range(COPIES)]
        peak = functools.reduce(jnp.maximum, levels)
        weights = [jnp.exp(level - peak) for level in levels]
        inv = 1.0 / sum(weights)
        spot = lax.broadcasted_iota(jnp.int32, (batch, heads, rows), 0) * heads
        spot = spot + lax.broadcasted_iota(jnp.int32, (batch, heads, rows), 1)
        here = lax.broadcasted_iota(jnp.int32, (batch, heads, rows), 2) == spot
        blocks = []
        for weight in weights:
            expanded = jnp.broadcast_to((weight * inv)[:, None, :], (batch, heads, rows))
            blocks.append(jnp.where(here, expanded, 0.0).reshape(rows, rows))
        mix = jnp.concatenate(blocks, axis=1)
        high = mix.astype(BF16)
        low = (mix - high.astype(F32)).astype(BF16)
        parts = all_out[...].reshape(COPIES * rows, DH)
        att_rows[...] = jnp.dot(high, parts, preferred_element_type=F32) + jnp.dot(
            low, parts, preferred_element_type=F32
        )
        attention = jnp.concatenate(
            [att_rows[pl.ds(h, batch, stride=heads), :] for h in range(heads)], axis=1
        ).astype(BF16)
        for core in range(n_c):
            proj_mine[core] = jnp.dot(
                attention, w_ref[core], preferred_element_type=F32
            ).astype(BF16)
        proj_all[x] = proj_mine[top]

        pl.semaphore_wait(side_sem.at[1], 2)
        for dx in sorted(range(n_x), key=lambda d: -min(d, n_x - d)):
            for core in range(n_c):
                if dx == 0 and core == top:
                    continue
                pltpu.make_async_remote_copy(
                    src_ref=proj_mine.at[core],
                    dst_ref=proj_all.at[x],
                    send_sem=c_send.at[core],
                    recv_sem=c_recv,
                    device_id={"head": lax.rem(x + dx, n_x), "sub": core},
                    device_id_type=MESH,
                ).start()
        wait_all(all_lse, (n_z - 1) * per, b_send.at[1])
        wait_all(all_out, n_z - 1, b_send.at[0])
        wait_all(proj_all, n_x, c_send.at[0])
        wait_all(proj_all, n_x - 1, c_send.at[top])
        wait_all(proj_all, n_x - 1, c_recv)

    pl.when(c != top)(other_core)
    pl.when(c == top)(top_core)
    summed = proj_all[0].astype(F32)
    for i in range(1, n_x):
        summed = summed + proj_all[i].astype(F32)
    out_ref[...] = summed.astype(out_ref.dtype)


def on_device(sizes, queries, key_cache, value_cache, seq_lengths, slot_owner, slot_page, out_weight):
    n_z, n_x, n_c = sizes
    batch, heads = queries.shape[0], queries.shape[1] // DH
    slots = key_cache.shape[0]
    rows = batch * heads
    width = out_weight.shape[1]
    sources = n_z // COPIES * n_c
    per = batch // (n_z // COPIES)
    assert key_cache.shape[2] == DH and rows == DH and n_c == 2
    hbm = pl.BlockSpec(memory_space=pltpu.HBM)
    dma = pltpu.SemaphoreType.DMA
    return pl.pallas_call(
        functools.partial(kernel, sizes),
        out_shape=pltpu.VMEM((batch, width), BF16),
        in_specs=[hbm] * 8,
        out_specs=pl.BlockSpec(memory_space=pltpu.VMEM),
        scratch_shapes=[
            pltpu.SMEM((batch,), jnp.int32),
            pltpu.SMEM((slots,), jnp.int32),
            pltpu.SMEM((slots,), jnp.int32),
            pltpu.VMEM((1, slots), jnp.int32),
            pltpu.VMEM(queries.shape, BF16),
            pltpu.VMEM(key_cache.shape, BF16),
            pltpu.VMEM(value_cache.shape, BF16),
            pltpu.VMEM((n_c, *out_weight.shape), BF16),
            pltpu.VMEM((rows, DH), F32),
            pltpu.VMEM((batch, heads, DH), F32),
            pltpu.VMEM((slots * heads, PAGE), F32),
            pltpu.VMEM((slots * heads, PAGE), F32),
            pltpu.VMEM((rows, slots * heads), BF16),
            pltpu.VMEM((batch, heads, rows), F32),
            pltpu.VMEM((batch, heads, rows), F32),
            pltpu.VMEM((rows, rows), F32),
            pltpu.VMEM((batch // per, per, heads, DH), BF16),
            pltpu.VMEM((batch, rows), F32),
            pltpu.VMEM((sources, per, heads, DH), BF16),
            pltpu.VMEM((sources * per, rows), F32),
            pltpu.VMEM((per, heads, DH), BF16),
            pltpu.VMEM((per, rows), F32),
            pltpu.VMEM((n_z, per, heads, DH), BF16),
            pltpu.VMEM((n_z * per, rows), F32),
            pltpu.VMEM((rows, DH), F32),
            pltpu.VMEM((n_c, batch, width), BF16),
            pltpu.VMEM((n_x, batch, width), BF16),
            dma((5,)),
            dma,
            dma,
            dma,
            dma((2,)),
            dma((2,)),
            dma((2,)),
            dma((2,)),
            dma((2,)),
            dma((n_c,)),
            dma,
            pltpu.SemaphoreType.REGULAR,
            pltpu.SemaphoreType.REGULAR((2,)),
        ],
        compiler_params=pltpu.CompilerParams(collective_id=0, has_side_effects=True),
        name="decode",
    )(
        seq_lengths,
        slot_owner,
        slot_page,
        slot_owner.reshape(1, slots),
        queries,
        key_cache,
        value_cache,
        out_weight,
    )


def solution(mesh):
    sizes = (mesh.shape["seq"], mesh.shape["head"], mesh.shape["sub"])
    in_specs = (
        P("rep", "head"),
        P(("rep", "seq", "sub"), None, "head"),
        P(("rep", "seq", "sub"), None, "head"),
        P("rep"),
        P(("rep", "seq", "sub")),
        P(("rep", "seq", "sub")),
        P("head", ("seq", "sub")),
    )
    out_specs = P("rep", ("seq", "sub"))
    return jax.shard_map(
        functools.partial(on_device, sizes),
        mesh=mesh,
        in_specs=in_specs,
        out_specs=out_specs,
        check_vma=False,
    )
```

```python
import functools

import jax
import jax.numpy as jnp
from jax import lax
from jax.experimental import pallas as pl
from jax.experimental.pallas import tpu as pltpu
from jax.sharding import PartitionSpec as P

DH = 128
PAGE = 128
NEG = -1e30
COPIES = 4
F32 = jnp.float32
BF16 = jnp.bfloat16
MESH = pl.DeviceIdType.MESH


def kernel(
    sizes,
    lengths_hbm,
    owners_hbm,
    numbers_hbm,
    owner_row_hbm,
    q_hbm,
    k_hbm,
    v_hbm,
    w_hbm,
    out_ref,
    lengths,
    owners,
    numbers,
    owner_row,
    q_ref,
    k_ref,
    v_ref,
    w_ref,
    q_rows,
    q_seq,
    peaks,
    masses,
    hits,
    seq_peak,
    seq_lse,
    lse_diag,
    part_out,
    part_lse,
    got_out,
    got_lse,
    own_out,
    own_lse,
    all_out,
    all_lse,
    att_rows,
    proj_mine,
    proj_all,
    small_sem,
    k_sem,
    v_sem,
    w_sem,
    w_pass,
    a_send,
    a_recv,
    b_send,
    b_recv,
    c_send,
    c_recv,
    far_sem,
    side_sem,
):
    n_z, n_x, n_c = sizes
    batch, heads, slots = lengths.shape[0], q_ref.shape[1] // DH, owners.shape[0]
    half = n_z // 2
    near = half // 2
    seg = n_z // COPIES
    per = batch // seg
    top = n_c - 1
    sources = seg * n_c
    z, x, c = lax.axis_index("seq"), lax.axis_index("head"), lax.axis_index("sub")
    rows = batch * heads

    def ring(offset):
        return lax.rem(z + offset + n_z, n_z)

    small = [
        pltpu.make_async_copy(src, dst, small_sem.at[i])
        for i, (src, dst) in enumerate(
            (
                (owners_hbm, owners),
                (lengths_hbm, lengths),
                (numbers_hbm, numbers),
                (owner_row_hbm, owner_row),
                (q_hbm, q_ref),
            )
        )
    ]
    k_load = pltpu.make_async_copy(k_hbm, k_ref, k_sem)
    v_load = pltpu.make_async_copy(v_hbm, v_ref, v_sem)
    w_load = pltpu.make_async_copy(w_hbm, w_ref.at[top], w_sem)
    for copy in small + [k_load, v_load]:
        copy.start()

    def wait_all(ref, count, sem):
        span = ref.at[pl.ds(0, count)]
        pltpu.make_async_copy(span, span, sem).wait()

    barrier = pltpu.get_barrier_semaphore()

    def greet(**where):
        pl.semaphore_signal(barrier, inc=1, device_id=where, device_id_type=MESH)

    @pl.when(c == top)
    def _():
        for dz in sorted(range(-near, near + 1), key=lambda d: -abs(d)):
            for core in range(n_c):
                if dz or core != top:
                    greet(seq=ring(dz), sub=core)
        for dx in (1, n_x - 1):
            greet(head=lax.rem(x + dx, n_x), sub=top)

    @pl.when(c != top)
    def _():
        for dx in (0, 1, n_x - 1):
            greet(head=lax.rem(x + dx, n_x), sub=top)

    greeted_top = 2 * near + (n_c - 1) + 2 * n_c
    greeted_other = 2 * near + 1

    for copy in small:
        copy.wait()

    lane = lax.broadcasted_iota(jnp.int32, (heads, rows), 1)
    sub = lax.broadcasted_iota(jnp.int32, (heads, rows), 0)
    diag = lane - sub

    for h in range(heads):
        q_rows[pl.ds(h, batch, stride=heads), :] = q_ref[:, h * DH : (h + 1) * DH].astype(F32)
    q_seq[...] = q_rows[...].reshape(batch, heads, DH)

    hit = (lax.broadcasted_iota(jnp.int32, (batch, slots), 0) == owner_row[...]).astype(BF16)
    spread_rows = lax.broadcasted_iota(jnp.int32, (slots, slots * heads), 0)
    spread_cols = lax.broadcasted_iota(jnp.int32, (slots, slots * heads), 1)
    spread = (spread_cols // heads == spread_rows).astype(BF16)
    wide = jnp.dot(hit, spread, preferred_element_type=F32)
    wide = jnp.broadcast_to(wide[:, None, :], (batch, heads, slots * heads))
    w_sub = lax.broadcasted_iota(jnp.int32, (batch, heads, slots * heads), 1)
    w_lane = lax.broadcasted_iota(jnp.int32, (batch, heads, slots * heads), 2)
    hits[...] = jnp.where(w_lane % heads == w_sub, wide, 0.0).reshape(rows, slots * heads).astype(BF16)

    scale = 1.0 / (float(DH) ** 0.5)
    pair_sub = lax.broadcasted_iota(jnp.int32, (2 * heads, PAGE), 0)
    pair_lane = lax.broadcasted_iota(jnp.int32, (2 * heads, PAGE), 1)
    first = pair_sub < heads

    probs = []
    peak_diag = jnp.full((heads, rows), NEG, F32)
    k_load.wait()
    for pair in range(slots // 2):
        a, b = 2 * pair, 2 * pair + 1
        own_a, own_b = owners[a], owners[b]
        q_pair = jnp.concatenate(
            [
                q_seq[own_a],
                q_seq[own_b],
            ],
            axis=0,
        ).astype(BF16)
        keys = k_ref[a : b + 1].reshape(2 * PAGE, DH)
        both = lax.dot_general(
            q_pair, keys, (((1,), (1,)), ((), ())), preferred_element_type=F32
        )
        scores = jnp.concatenate([both[:heads, :PAGE], both[heads:, PAGE:]], axis=0) * scale
        live_a = jnp.clip(lengths[own_a] - numbers[a] * PAGE, 0, PAGE)
        live_b = jnp.clip(lengths[own_b] - numbers[b] * PAGE, 0, PAGE)
        scores = jnp.where(pair_lane < jnp.where(first, live_a, live_b), scores, NEG)
        peak = jnp.max(scores, axis=1, keepdims=True)
        prob = jnp.exp(scores - peak).astype(BF16)
        mass = jnp.sum(prob.astype(F32), axis=1, keepdims=True)
        peak = jnp.broadcast_to(peak, (2 * heads, PAGE))
        mass = jnp.broadcast_to(mass, (2 * heads, PAGE))
        peaks[pl.ds(a * heads, 2 * heads), :] = peak
        masses[pl.ds(a * heads, 2 * heads), :] = mass
        probs.append(prob)
        peak_diag = jnp.maximum(peak_diag, jnp.where(diag == own_a * heads, peak[:heads], NEG))
        peak_diag = jnp.maximum(peak_diag, jnp.where(diag == own_b * heads, peak[heads:], NEG))


    @pl.when(c == top)
    def _():
        pl.semaphore_wait(barrier, greeted_top)
        for dz in (-near, near):
            pl.semaphore_signal(far_sem, inc=1, device_id={"seq": ring(dz)}, device_id_type=MESH)
        for dx in (1, n_x - 1):
            pl.semaphore_signal(
                side_sem.at[0], inc=1, device_id={"head": lax.rem(x + dx, n_x)}, device_id_type=MESH
            )

    @pl.when(c != top)
    def _():
        pl.semaphore_wait(barrier, greeted_other)

    v_load.wait()

    def by_sequence(row_values, ref):
        for b in range(batch):
            mine = jnp.max(
                jnp.where(lane // heads == b, row_values, 2 * NEG), axis=1, keepdims=True
            )
            ref[b] = jnp.broadcast_to(mine, (heads, rows))

    by_sequence(peak_diag, seq_peak)
    total = jnp.zeros((heads, rows), F32)
    factors = []
    for s in range(slots):
        span = pl.ds(s * heads, heads)
        factors.append(jnp.exp(peaks[span, :] - seq_peak[owners[s]]))
        total = total + jnp.where(diag == owners[s] * heads, factors[s] * masses[span, :], 0.0)
    lse = jnp.where(
        total > 0.0, peak_diag + jnp.log(jnp.where(total > 0.0, total, 1.0)), NEG
    )
    by_sequence(lse, seq_lse)

    for b in range(batch):
        lse_diag[pl.ds(b * heads, heads), :] = jnp.where(lane % heads == sub, seq_lse[b], 0.0)
    tiled = lse_diag[pl.ds(0, batch, stride=heads), :]
    for h in range(1, heads):
        tiled = tiled + lse_diag[pl.ds(h, batch, stride=heads), :]
    part_lse[...] = tiled

    high, low = [], []
    for pair in range(slots // 2):
        a, b = 2 * pair, 2 * pair + 1
        prob = probs[pair]
        block = jnp.concatenate(
            [
                jnp.where(first, prob, jnp.zeros_like(prob)),
                jnp.where(first, jnp.zeros_like(prob), prob),
            ],
            axis=1,
        )
        values = v_ref[a : b + 1].reshape(2 * PAGE, DH)
        page_out = jnp.dot(block, values, preferred_element_type=F32)
        page_out = page_out * jnp.concatenate([factors[a], factors[b]], axis=0)
        high.append(page_out.astype(BF16))
        low.append((page_out - high[-1].astype(F32)).astype(BF16))
    hit = hits[...]
    mine = jnp.dot(hit, jnp.concatenate(high, axis=0), preferred_element_type=F32)
    mine = mine + jnp.dot(hit, jnp.concatenate(low, axis=0), preferred_element_type=F32)
    mine = mine * jnp.exp(seq_peak[...] - seq_lse[...]).reshape(rows, rows)
    part_out[...] = mine.astype(BF16).reshape(seg, per, heads, DH)

    def send_parts(core):
        sent = 0
        for dz in sorted(range(-(seg // 2), seg // 2), key=lambda d: -abs(d)):
            target = lax.rem(ring(dz), seg)
            slot = (seg // 2 - 1 - dz) * n_c + core
            src_rows, dst_rows = pl.ds(target * per, per), pl.ds(slot * per, per)
            if dz == 0 and core == top:
                got_out[slot] = part_out[target]
                got_lse[dst_rows, :] = part_lse[src_rows, :]
                continue
            for k, (src, dst) in enumerate(
                (
                    (part_out.at[target], got_out.at[slot]),
                    (part_lse.at[src_rows, :], got_lse.at[dst_rows, :]),
                )
            ):
                pltpu.make_async_remote_copy(
                    src_ref=src,
                    dst_ref=dst,
                    send_sem=a_send.at[k],
                    recv_sem=a_recv.at[k],
                    device_id={"seq": ring(dz), "sub": top},
                    device_id_type=MESH,
                ).start()
            sent += 1
        return sent

    def other_core():
        sent = send_parts(0)
        weights = pltpu.make_async_remote_copy(
            src_ref=w_hbm,
            dst_ref=w_ref.at[0],
            send_sem=w_pass.at[0],
            recv_sem=w_pass.at[1],
            device_id={"sub": top},
            device_id_type=MESH,
        )
        weights.start()
        wait_all(part_lse, sent * per, a_send.at[1])
        wait_all(part_out, sent, a_send.at[0])
        weights.wait_send()
        wait_all(proj_all, n_x, c_recv)

    def top_core():
        sent = send_parts(top)
        w_load.start()
        wait_all(got_lse, (sources - 1) * per, a_recv.at[1])
        wait_all(got_out, sources - 1, a_recv.at[0])

        wide_rows = rows * n_c
        s_sub = lax.broadcasted_iota(jnp.int32, (sources, wide_rows), 0)
        s_lane = lax.broadcasted_iota(jnp.int32, (sources, wide_rows), 1)
        m_lane = lax.broadcasted_iota(jnp.int32, (heads, wide_rows), 1)
        m_sub = lax.broadcasted_iota(jnp.int32, (heads, wide_rows), 0)
        mixes = []
        for i in range(per):
            levels = got_lse[pl.ds(i, sources, stride=per), :]
            peak = jnp.max(levels, axis=0, keepdims=True)
            weight = jnp.exp(levels - peak)
            norm = jnp.sum(weight, axis=0, keepdims=True)
            weight = jnp.concatenate([weight / norm] * n_c, axis=1)
            flat = jnp.sum(
                jnp.where(s_lane // heads == s_sub * per + i, weight, 0.0), axis=0, keepdims=True
            )
            mixes.append(jnp.where(m_lane % heads == m_sub, jnp.broadcast_to(flat, (heads, wide_rows)), 0.0))
            own_lse[pl.ds(i, 1), :] = peak + jnp.log(norm)
        mix = jnp.concatenate(mixes, axis=0)
        high = mix.astype(BF16)
        low = (mix - high.astype(F32)).astype(BF16)
        parts = got_out[...].reshape(wide_rows, DH)
        both = jnp.dot(
            jnp.concatenate([high, low], axis=0), parts, preferred_element_type=F32
        )
        own = both[: per * heads] + both[per * heads :]
        own_out[...] = own.astype(BF16).reshape(per, heads, DH)

        pl.semaphore_wait(far_sem, 2)
        b_rows = pl.ds(z * per, per)
        all_out[z] = own_out[...]
        all_lse[b_rows, :] = own_lse[...]
        for dz in sorted(range(-half + 1, half + 1), key=lambda d: -abs(d)):
            if dz == 0:
                continue
            for k, (src, dst) in enumerate(
                ((own_out, all_out.at[z]), (own_lse, all_lse.at[b_rows, :]))
            ):
                pltpu.make_async_remote_copy(
                    src_ref=src,
                    dst_ref=dst,
                    send_sem=b_send.at[k],
                    recv_sem=b_recv.at[k],
                    device_id={"seq": ring(dz)},
                    device_id_type=MESH,
                ).start()
        pl.semaphore_wait(side_sem.at[0], 2)
        for dx in (2, n_x - 2):
            pl.semaphore_signal(
                side_sem.at[1], inc=1, device_id={"head": lax.rem(x + dx, n_x)}, device_id_type=MESH
            )
        w_load.wait()
        pltpu.make_async_copy(w_ref.at[0], w_ref.at[0], w_pass.at[1]).wait()
        wait_all(part_lse, sent * per, a_send.at[1])
        wait_all(part_out, sent, a_send.at[0])
        wait_all(all_lse, (n_z - 1) * per, b_recv.at[1])
        wait_all(all_out, n_z - 1, b_recv.at[0])

        levels = [all_lse[i * batch : (i + 1) * batch, :] for i in range(COPIES)]
        peak = functools.reduce(jnp.maximum, levels)
        weights = [jnp.exp(level - peak) for level in levels]
        inv = 1.0 / sum(weights)
        spot = lax.broadcasted_iota(jnp.int32, (batch, heads, rows), 0) * heads
        spot = spot + lax.broadcasted_iota(jnp.int32, (batch, heads, rows), 1)
        here = lax.broadcasted_iota(jnp.int32, (batch, heads, rows), 2) == spot
        blocks = []
        for weight in weights:
            expanded = jnp.broadcast_to((weight * inv)[:, None, :], (batch, heads, rows))
            blocks.append(jnp.where(here, expanded, 0.0).reshape(rows, rows))
        mix = jnp.concatenate(blocks, axis=1)
        high = mix.astype(BF16)
        low = (mix - high.astype(F32)).astype(BF16)
        parts = all_out[...].reshape(COPIES * rows, DH)
        both = jnp.dot(
            jnp.concatenate([high, low], axis=0), parts, preferred_element_type=F32
        )
        att_rows[...] = both[:rows] + both[rows:]
        attention = jnp.concatenate(
            [att_rows[pl.ds(h, batch, stride=heads), :] for h in range(heads)], axis=1
        ).astype(BF16)
        for core in range(n_c):
            proj_mine[core] = jnp.dot(
                attention, w_ref[core], preferred_element_type=F32
            ).astype(BF16)
        proj_all[x] = proj_mine[top]

        pl.semaphore_wait(side_sem.at[1], 2)
        for dx in sorted(range(n_x), key=lambda d: -min(d, n_x - d)):
            for core in range(n_c):
                if dx == 0 and core == top:
                    continue
                pltpu.make_async_remote_copy(
                    src_ref=proj_mine.at[core],
                    dst_ref=proj_all.at[x],
                    send_sem=c_send.at[core],
                    recv_sem=c_recv,
                    device_id={"head": lax.rem(x + dx, n_x), "sub": core},
                    device_id_type=MESH,
                ).start()
        wait_all(all_lse, (n_z - 1) * per, b_send.at[1])
        wait_all(all_out, n_z - 1, b_send.at[0])
        wait_all(proj_all, n_x, c_send.at[0])
        wait_all(proj_all, n_x - 1, c_send.at[top])
        wait_all(proj_all, n_x - 1, c_recv)

    pl.when(c != top)(other_core)
    pl.when(c == top)(top_core)
    summed = proj_all[0].astype(F32)
    for i in range(1, n_x):
        summed = summed + proj_all[i].astype(F32)
    out_ref[...] = summed.astype(out_ref.dtype)


def on_device(sizes, queries, key_cache, value_cache, seq_lengths, slot_owner, slot_page, out_weight):
    n_z, n_x, n_c = sizes
    batch, heads = queries.shape[0], queries.shape[1] // DH
    slots = key_cache.shape[0]
    rows = batch * heads
    width = out_weight.shape[1]
    sources = n_z // COPIES * n_c
    per = batch // (n_z // COPIES)
    assert key_cache.shape[2] == DH and rows == DH and n_c == 2
    hbm = pl.BlockSpec(memory_space=pltpu.HBM)
    dma = pltpu.SemaphoreType.DMA
    return pl.pallas_call(
        functools.partial(kernel, sizes),
        out_shape=pltpu.VMEM((batch, width), BF16),
        in_specs=[hbm] * 8,
        out_specs=pl.BlockSpec(memory_space=pltpu.VMEM),
        scratch_shapes=[
            pltpu.SMEM((batch,), jnp.int32),
            pltpu.SMEM((slots,), jnp.int32),
            pltpu.SMEM((slots,), jnp.int32),
            pltpu.VMEM((1, slots), jnp.int32),
            pltpu.VMEM(queries.shape, BF16),
            pltpu.VMEM(key_cache.shape, BF16),
            pltpu.VMEM(value_cache.shape, BF16),
            pltpu.VMEM((n_c, *out_weight.shape), BF16),
            pltpu.VMEM((rows, DH), F32),
            pltpu.VMEM((batch, heads, DH), F32),
            pltpu.VMEM((slots * heads, PAGE), F32),
            pltpu.VMEM((slots * heads, PAGE), F32),
            pltpu.VMEM((rows, slots * heads), BF16),
            pltpu.VMEM((batch, heads, rows), F32),
            pltpu.VMEM((batch, heads, rows), F32),
            pltpu.VMEM((rows, rows), F32),
            pltpu.VMEM((batch // per, per, heads, DH), BF16),
            pltpu.VMEM((batch, rows), F32),
            pltpu.VMEM((sources, per, heads, DH), BF16),
            pltpu.VMEM((sources * per, rows), F32),
            pltpu.VMEM((per, heads, DH), BF16),
            pltpu.VMEM((per, rows), F32),
            pltpu.VMEM((n_z, per, heads, DH), BF16),
            pltpu.VMEM((n_z * per, rows), F32),
            pltpu.VMEM((rows, DH), F32),
            pltpu.VMEM((n_c, batch, width), BF16),
            pltpu.VMEM((n_x, batch, width), BF16),
            dma((5,)),
            dma,
            dma,
            dma,
            dma((2,)),
            dma((2,)),
            dma((2,)),
            dma((2,)),
            dma((2,)),
            dma((n_c,)),
            dma,
            pltpu.SemaphoreType.REGULAR,
            pltpu.SemaphoreType.REGULAR((2,)),
        ],
        compiler_params=pltpu.CompilerParams(collective_id=0, has_side_effects=True),
        name="decode",
    )(
        seq_lengths,
        slot_owner,
        slot_page,
        slot_owner.reshape(1, slots),
        queries,
        key_cache,
        value_cache,
        out_weight,
    )


def solution(mesh):
    sizes = (mesh.shape["seq"], mesh.shape["head"], mesh.shape["sub"])
    in_specs = (
        P("rep", "head"),
        P(("rep", "seq", "sub"), None, "head"),
        P(("rep", "seq", "sub"), None, "head"),
        P("rep"),
        P(("rep", "seq", "sub")),
        P(("rep", "seq", "sub")),
        P("head", ("seq", "sub")),
    )
    out_specs = P("rep", ("seq", "sub"))
    return jax.shard_map(
        functools.partial(on_device, sizes),
        mesh=mesh,
        in_specs=in_specs,
        out_specs=out_specs,
        check_vma=False,
    )
```
